32 devices in a mesh: gx: 8 (over z, x), col: 4 (over y, core).
Axes of the slice: x: 2, y: 2, z: 4, core: 2. Of those that a mesh axis runs over, the one named last changes fastest.
Arguments:
- grid_field: bfloat16 [64, 32, 256, 128], P('col', 'gx'), may hold values from -6 to 6
- tucker_core: float32 [2, 32, 32, 8, 8, 4], P(None, 'col'), may hold values from -0.5 to 0.5
- in_factor: float32 [64, 32], P('col'), may hold values from -0.75 to 0.75
- out_factor: float32 [64, 32], P('col'), may hold values from -1 to 1
- x_factor: float32 [32, 8], replicated, may hold values from -4 to 4
- y_factor: float32 [32, 8], replicated, may hold values from -4 to 4
- z_factor: float32 [16, 4], replicated, may hold values from -4 to 4
- kx_reach: int32 [32, 16], replicated, may hold values from 1 to 17
Outputs:
- spectral_out: bfloat16 [64, 32, 256, 128], P('col', 'gx')
The draws below stay inside these ranges and needn't reach their ends.
All inputs are finite; a program needn't handle non-finite values.
Results may differ from the reference program's by a relative error of at most 0.001.
Values sent between devices are 32-bit elements; how exact they have to be, the bound alone decides.
A program may use at most 64 MiB of HBM per device.

```python
import jax
import jax.numpy as jnp
from jax import lax

C = 64
R_IN = 32
R_OUT = 32
RX = 8
RY = 8
RZ = 4
KX = 32
KY = 32
KZ = 16
NY = 256
NZ = 128
NX = 32


def set_ends(result, key, low, top_value):
    dims = result.shape
    spot = [jax.random.randint(jax.random.fold_in(key, axis), (), 0, dims[axis]) for axis in range(len(dims))]
    result = result.at[tuple(spot)].set(low)
    longest = dims.index(max(dims))
    spot[longest] = (spot[longest] + 1) % dims[longest]
    return result.at[tuple(spot)].set(top_value)


def steps_of(key, shape, split, low, top_value):
    loudness, own = 1.0, jax.random.fold_in(key, 6)
    for axis_at, shards_of in split:
        steps = jnp.exp(jax.random.uniform(jax.random.fold_in(own, axis_at), (shards_of,), jnp.float32, low / len(split), top_value / len(split)))
        loudness = loudness * jnp.repeat(steps, shape[axis_at] // shards_of).reshape([-1 if axis == axis_at else 1 for axis in range(len(shape))])
    return loudness


def noise(own_key, extent, scale, reach, pieces=(), kind=jnp.bfloat16):
    values = jax.random.normal(own_key, extent, jnp.float32) * scale
    if len(pieces) > 0:
        values = steps_of(own_key, extent, pieces, -0.22, 0.18) * values
    return jnp.clip(values, min=-reach, max=reach).astype(kind)


def setup_inputs(seed: int = 0) -> dict:
    streams_of = jax.random.split(jax.random.key(seed), 9)
    grid_field = noise(streams_of[0], (C, NX, NY, NZ), 1.0, 6.0, ((0, 4), (1, 8)))
    tucker_core = noise(streams_of[1], (2, R_IN, R_OUT, RX, RY, RZ), (max(1, KX * KY * KZ * R_IN * RX * RY * RZ // (NX * NY * NZ))) ** -0.5, 0.5, ((1, 4),), jnp.float32)
    in_factor = noise(streams_of[2], (C, R_IN), C ** -0.5, 0.75, ((0, 4),), jnp.float32)
    out_factor = noise(streams_of[3], (C, R_OUT), R_OUT ** -0.5, 1.0, ((0, 4),), jnp.float32)
    x_factor = noise(streams_of[4], (KX, RX), 1.0, 4.0, (), jnp.float32)
    y_factor = noise(streams_of[5], (KY, RY), 1.0, 4.0, (), jnp.float32)
    z_factor = noise(streams_of[6], (KZ, RZ), 1.0, 4.0, (), jnp.float32)
    kx_reach = set_ends(jax.random.randint(streams_of[7], (KY, KZ), 1, KX // 2 + 2), jax.random.fold_in(streams_of[7], 1), 1, (KX // 2 + 2) - 1).astype(jnp.int32)
    return {"grid_field": grid_field, "tucker_core": tucker_core, "in_factor": in_factor, "out_factor": out_factor, "x_factor": x_factor, "y_factor": y_factor, "z_factor": z_factor, "kx_reach": kx_reach}


def slot_freq(slot_count):
    slot_index = jnp.arange(slot_count, dtype=jnp.int32)
    return jnp.where(slot_index < slot_count // 2, slot_index, slot_index - slot_count)


def forward_one(channel):
    values = channel.astype(jnp.float32)
    spectrum = jnp.fft.rfft(values, axis=2, norm="ortho")[:, :, :KZ]
    spectrum = jnp.fft.fft(spectrum, axis=1, norm="ortho")
    spectrum = jnp.concatenate([spectrum[:, :KY // 2], spectrum[:, NY - KY // 2:]], axis=1)
    spectrum = jnp.fft.fft(spectrum, axis=0, norm="ortho")
    spectrum = jnp.concatenate([spectrum[:KX // 2], spectrum[NX - KX // 2:]], axis=0)
    return jnp.real(spectrum), jnp.imag(spectrum)


def inverse_one(pair_parts):
    real_part, imag_part = pair_parts
    values = real_part + 1j * imag_part
    zero_fill = jnp.zeros((NX - KX, KY, KZ), values.dtype)
    values = jnp.concatenate([values[:KX // 2], zero_fill, values[KX // 2:]], axis=0)
    values = jnp.fft.ifft(values, axis=0, norm="ortho")
    zero_fill = jnp.zeros((NX, NY - KY, KZ), values.dtype)
    values = jnp.concatenate([values[:, :KY // 2], zero_fill, values[:, KY // 2:]], axis=1)
    values = jnp.fft.ifft(values, axis=1, norm="ortho")
    zero_fill = jnp.zeros((NX, NY, NZ // 2 + 1 - KZ), values.dtype)
    values = jnp.concatenate([values, zero_fill], axis=2)
    return jnp.fft.irfft(values, n=NZ, axis=2, norm="ortho").astype(jnp.bfloat16)


def reference(grid_field, tucker_core, in_factor, out_factor, x_factor, y_factor, z_factor, kx_reach):
    highest = lax.Precision.HIGHEST
    real_spec, imag_spec = lax.map(forward_one, grid_field)
    kept_mask = (jnp.abs(slot_freq(KX))[:, None, None] < kx_reach[None, :, :]).astype(jnp.float32)
    rank_re = jnp.einsum('cr,cijl->rijl', in_factor, real_spec, precision=highest) * kept_mask
    rank_im = jnp.einsum('cr,cijl->rijl', in_factor, imag_spec, precision=highest) * kept_mask

    def per_row(row_items):
        row_re, row_im, y_row = row_items
        partial_value = jnp.einsum('prsabe,b->prsae', tucker_core, y_row, precision=highest)
        kernel = jnp.einsum('prsae,ia,le->prsil', partial_value, x_factor, z_factor, precision=highest)
        mixed_re = (jnp.einsum('rsil,ril->sil', kernel[0], row_re, precision=highest)
                    - jnp.einsum('rsil,ril->sil', kernel[1], row_im, precision=highest))
        mixed_im = (jnp.einsum('rsil,ril->sil', kernel[0], row_im, precision=highest)
                    + jnp.einsum('rsil,ril->sil', kernel[1], row_re, precision=highest))
        out_re = jnp.einsum('os,sil->oil', out_factor, mixed_re, precision=highest)
        out_im = jnp.einsum('os,sil->oil', out_factor, mixed_im, precision=highest)
        return out_re, out_im

    out_re, out_im = lax.map(per_row, (jnp.moveaxis(rank_re, 2, 0), jnp.moveaxis(rank_im, 2, 0), y_factor))
    out_re = jnp.transpose(out_re, (1, 2, 0, 3))
    out_im = jnp.transpose(out_im, (1, 2, 0, 3))
    return lax.map(inverse_one, (out_re, out_im))
```

```python
import functools
import math

import jax
import jax.numpy as jnp
import numpy as np
from jax import lax
from jax.experimental import pallas as pl
from jax.experimental.pallas import tpu as pltpu
from jax.sharding import PartitionSpec as P

MESH = pl.DeviceIdType.MESH
VMEM = pl.BlockSpec(memory_space=pltpu.VMEM)
F32 = jnp.float32
BF16 = jnp.bfloat16


def slot_freq(slot_count):
    slot_index = jnp.arange(slot_count, dtype=jnp.int32)
    return jnp.where(slot_index < slot_count // 2, slot_index, slot_index - slot_count)


def phase_table(positions, extent, slot_count, direction):
    phase_steps = positions[:, None] * slot_freq(slot_count)[None, :] % extent
    radians = 2.0 * math.pi / extent * phase_steps.astype(jnp.float32)
    norm_scale = 1.0 / math.sqrt(extent)
    cosine = jnp.cos(radians) * norm_scale
    sine_part = direction * jnp.sin(radians) * norm_scale
    return jnp.stack([jnp.stack([cosine, -sine_part], 1), jnp.stack([sine_part, cosine], 1)], 1)


def z_tables(grid_z, modes_z):
    z_index = jnp.arange(grid_z, dtype=jnp.int32)
    kz_index = jnp.arange(modes_z, dtype=jnp.int32)
    phase_steps = z_index[:, None] * kz_index[None, :] % grid_z
    radians = 2.0 * math.pi / grid_z * phase_steps.astype(jnp.float32)
    norm_scale = 1.0 / math.sqrt(grid_z)
    cosine = jnp.cos(radians) * norm_scale
    sine_part = jnp.sin(radians) * norm_scale
    forward = jnp.stack([cosine, -sine_part], 1)
    weight = jnp.where(kz_index == 0, 1.0, 2.0).astype(jnp.float32)
    backward = jnp.stack([(cosine * weight[None, :]).T, -(sine_part * weight[None, :]).T], 0)
    return (forward, backward)


def plain_device(
    grid_field, tucker_core, in_factor, out_factor, x_factor, y_factor, z_factor, kx_reach
):
    highest = lax.Precision.HIGHEST
    channels, planes, grid_y, grid_z = grid_field.shape
    modes_x = x_factor.shape[0]
    modes_y = y_factor.shape[0]
    modes_z = z_factor.shape[0]
    width_gx = lax.axis_size("gx")
    grid_x = planes * width_gx
    columns = modes_y * modes_z
    col_dev = columns // width_gx
    slab_index = lax.axis_index("gx")
    z_forward, z_backward = z_tables(grid_z, modes_z)
    y_forward = phase_table(jnp.arange(grid_y, dtype=jnp.int32), grid_y, modes_y, 1.0)
    x_forward = phase_table(jnp.arange(grid_x, dtype=jnp.int32), grid_x, modes_x, 1.0)
    values = grid_field.astype(jnp.float32)
    z_spectrum = jnp.einsum("cxyz,zpl->cxply", values, z_forward, precision=highest)
    y_spectrum = jnp.einsum("cxply,ypqj->qcxjl", z_spectrum, y_forward, precision=highest)
    y_spectrum = y_spectrum.reshape(2, channels, planes, columns)
    first_col = slab_index * col_dev
    reach_dev = lax.dynamic_slice_in_dim(kx_reach.reshape(-1), first_col, col_dev)
    kept_mask = (jnp.abs(slot_freq(modes_x))[:, None] < reach_dev[None, :]).astype(jnp.float32)
    arrived = lax.all_to_all(y_spectrum, "gx", split_axis=3, concat_axis=2, tiled=True)
    spectrum = jnp.einsum("pcxm,xpqk->qckm", arrived, x_forward, precision=highest)
    partial_value = jnp.einsum("qckm,cr->qrkm", spectrum, in_factor, precision=highest)
    amplitude = lax.psum_scatter(partial_value, "col", scatter_dimension=1, tiled=True)
    amplitude = amplitude * kept_mask[None, None]
    column = first_col + jnp.arange(col_dev, dtype=jnp.int32)
    pick_y = (column[:, None] // modes_z == jnp.arange(modes_y, dtype=jnp.int32)[None, :]).astype(
        jnp.float32
    )
    pick_z = (column[:, None] % modes_z == jnp.arange(modes_z, dtype=jnp.int32)[None, :]).astype(
        jnp.float32
    )
    y_rows = jnp.dot(pick_y, y_factor, precision=highest)
    z_rows = jnp.dot(pick_z, z_factor, precision=highest)
    core_cols = jnp.einsum("prsabe,mb,me->prsam", tucker_core, y_rows, z_rows, precision=highest)
    kernel = jnp.einsum("prsam,ka->prskm", core_cols, x_factor, precision=highest)
    mixed_re = jnp.einsum("rskm,rkm->skm", kernel[0], amplitude[0], precision=highest) - jnp.einsum(
        "rskm,rkm->skm", kernel[1], amplitude[1], precision=highest
    )
    mixed_im = jnp.einsum("rskm,rkm->skm", kernel[0], amplitude[1], precision=highest) + jnp.einsum(
        "rskm,rkm->skm", kernel[1], amplitude[0], precision=highest
    )
    mixed_sum = lax.psum(jnp.stack([mixed_re, mixed_im]), "col")
    out_spec = jnp.einsum("os,qskm->qokm", out_factor, mixed_sum, precision=highest)
    x_backward = phase_table(jnp.arange(grid_x, dtype=jnp.int32), grid_x, modes_x, -1.0)
    x_values = jnp.einsum("pckm,xpqk->qcxm", out_spec, x_backward, precision=highest)
    returned = lax.all_to_all(x_values, "gx", split_axis=2, concat_axis=3, tiled=True)
    returned = returned.reshape(2, channels, planes, modes_y, modes_z)
    y_backward = phase_table(jnp.arange(grid_y, dtype=jnp.int32), grid_y, modes_y, -1.0)
    y_values = jnp.einsum("pcxjl,ypqj->cxqly", returned, y_backward, precision=highest)
    result = jnp.einsum("cxqly,qlz->cxyz", y_values, z_backward, precision=highest)
    return result.astype(jnp.bfloat16)


def split_np(table):
    high = table.astype(np.float32).astype(BF16)
    low = (table - high.astype(np.float64)).astype(np.float32).astype(BF16)
    return high, low


def split(values):
    high = values.astype(BF16)
    return high, (values - high.astype(F32)).astype(BF16)


def freqs(slots):
    index = np.arange(slots)
    return np.where(index < slots // 2, index, index - slots)


def waves(extent, frequencies):
    steps = np.arange(extent)[:, None] * frequencies[None, :] % extent
    angle = 2.0 * np.pi / extent * steps
    return np.cos(angle) / math.sqrt(extent), np.sin(angle) / math.sqrt(extent)


def dot(a, b):
    return jnp.dot(a, b, preferred_element_type=F32)


def forward_tables(grid_y, grid_z, modes_y, modes_z, planes):
    cos_y, sin_y = waves(grid_y, freqs(modes_y))
    high, low = split_np(np.concatenate([cos_y.T, -sin_y.T], 0))
    y_table = np.concatenate([high, low], 0)
    cos_z, sin_z = waves(grid_z, np.arange(modes_z))
    table = np.zeros((planes, 2, grid_z, modes_z, planes, 2))
    for plane in range(planes):
        table[plane, 0, :, :, plane, 0] = cos_z
        table[plane, 0, :, :, plane, 1] = -sin_z
        table[plane, 1, :, :, plane, 0] = sin_z
        table[plane, 1, :, :, plane, 1] = cos_z
    high, low = split_np(table.reshape(planes * 2 * grid_z, -1))
    return y_table, np.concatenate([high, low], 1)


def inverse_tables(grid_y, grid_z, modes_y, modes_z, planes, halves):
    cos_y, sin_y = waves(grid_y, freqs(modes_y))
    high, low = split_np(np.concatenate([cos_y, -sin_y], 1))
    y_table = np.concatenate([high, high, low], 1)
    cos_z, sin_z = waves(grid_z, np.arange(modes_z))
    weight = np.where(np.arange(modes_z) == 0, 1.0, 2.0)
    cos_z, sin_z = (cos_z * weight).T, (sin_z * weight).T
    table = np.zeros((modes_z, planes, 2, planes, 2, grid_z))
    for plane in range(planes):
        table[:, plane, 0, plane, 0, :] = cos_z
        table[:, plane, 1, plane, 0, :] = -sin_z
        table[:, plane, 0, plane, 1, :] = sin_z
        table[:, plane, 1, plane, 1, :] = cos_z
    high, low = split_np(table.reshape(halves, modes_z // halves * planes * 2, -1))
    return y_table, np.concatenate([high, high, low], 1)


def x_tables(grid_x, modes_x):
    cos_x, sin_x = waves(grid_x, freqs(modes_x))
    real = np.stack([cos_x.T, sin_x.T], 2).reshape(modes_x, -1)
    imag = np.stack([-sin_x.T, cos_x.T], 2).reshape(modes_x, -1)
    high, low = split_np(np.concatenate([real, imag, -imag, real], 0))
    forward = np.concatenate([high, high, low], 1)
    real = np.concatenate([cos_x, -sin_x], 1)
    imag = np.concatenate([sin_x, cos_x], 1)
    high, low = split_np(np.stack([real, imag], 1).reshape(grid_x * 2, -1))
    backward = np.concatenate([high, high, low], 1)
    return forward, backward


def selectors(width_col, rank_in, rank_x, rank_y, rank_z, rank_out):
    wide = np.arange(rank_in * rank_x)
    x_pick = wide % rank_x == np.arange(rank_x)[:, None]
    in_pick = wide // rank_x == np.arange(rank_in)[:, None]
    slim = np.arange(rank_z * rank_out)
    z_pick = slim // rank_out == np.arange(rank_z)[:, None]
    out_pick = slim % rank_out == np.arange(rank_out)[:, None]
    core_in = np.arange(rank_x * rank_y * rank_z)
    y_pick = core_in // rank_z % rank_y == np.arange(rank_y)[:, None]
    core_out = np.arange(rank_z * width_col * rank_x)
    same_x = core_in // (rank_y * rank_z) == core_out[:, None] % rank_x
    same_z = core_in % rank_z == core_out[:, None] // (width_col * rank_x)
    picks = (x_pick, in_pick, z_pick, out_pick, y_pick, same_x & same_z)
    return [pick.astype(np.float32) for pick in picks]


def spread(values, pick, dim):
    return lax.dot_general(
        values, pick, (((dim,), (0,)), ((), ())), precision=lax.Precision.HIGHEST,
        preferred_element_type=F32,
    )


HALVES = 2


def fused_kernel(
    width_gx, width_col, field_hbm, core_hbm, in_hbm, out_hbm, x_hbm, y_hbm, z_hbm, reach_hbm,
    x_pick_hbm, in_pick_hbm, z_pick_hbm, out_pick_hbm, y_pick_hbm, same_hbm, y_table_hbm,
    z_table_hbm, fore_hbm, back_hbm, z_back_hbm, y_back_hbm, high_out, low_out, y_back_ref, field,
    core_in, in_ref, out_ref, x_ref, y_ref, z_ref, reach_ref, x_pick_ref, in_pick_ref, z_pick_ref,
    out_pick_ref, y_pick_ref, same_ref, y_table_ref, z_table_ref, fore_ref, back_ref, z_back_ref,
    y_high, y_low, values_ref, spec, arrived, cores, cores_in, factor, factors, kept_ref, rank_ref,
    high_ref, low_ref, plane_ref, result, returned, partial_ref, field_sems, load_sems, sends, recvs,
    core_sends, core_recvs, factor_sends, factor_recvs, back_sends, back_recvs,
):
    count = width_gx * width_col
    my_gx, my_col = lax.axis_index("gx"), lax.axis_index("col")
    me = my_gx * width_col + my_col
    channels, planes, _, grid_z = field.shape
    _, modes_y, group, lanes = spec.shape
    modes_x, modes_z = x_ref.shape[1], z_ref.shape[1]
    barrier = pltpu.get_barrier_semaphore()
    gx_steps = sorted(range(width_gx), key=lambda step: min(step, width_gx - step))
    col_steps = range(width_col)

    def slab_at(step):
        return lax.rem(my_gx + step, width_gx)

    def col_at(step):
        return lax.rem(my_col + step, width_col)

    for gx_step in gx_steps:
        for col_step in col_steps:
            if gx_step or col_step:
                pl.semaphore_signal(
                    barrier, inc=1, device_id=(slab_at(gx_step), col_at(col_step)),
                    device_id_type=MESH,
                )

    def fetch(channel):
        return pltpu.make_async_copy(
            field_hbm.at[channel], field.at[channel], field_sems.at[channel]
        )

    sources = [
        y_table_hbm, z_table_hbm, core_hbm, y_hbm, y_pick_hbm, same_hbm, in_hbm, out_hbm,
        in_pick_hbm, out_pick_hbm, x_hbm, z_hbm, reach_hbm, x_pick_hbm, z_pick_hbm, fore_hbm,
        back_hbm, z_back_hbm, y_back_hbm,
    ]
    targets = [
        y_table_ref, z_table_ref, core_in, y_ref, y_pick_ref, same_ref, in_ref, out_ref,
        in_pick_ref, out_pick_ref, x_ref, z_ref, reach_ref, x_pick_ref, z_pick_ref, fore_ref,
        back_ref, z_back_ref, y_back_ref,
    ]
    loads = [
        pltpu.make_async_copy(source, target, load_sems.at[index])
        for index, (source, target) in enumerate(zip(sources, targets))
    ]
    loads[0].start()

    def begin(channel, carry):
        fetch(channel).start()
        return carry

    lax.fori_loop(0, channels, begin, 0)
    for load in loads[1:]:
        load.start()

    def remote(source, target, send_sem, recv_sem, device):
        return pltpu.make_async_remote_copy(
            src_ref=source, dst_ref=target, send_sem=send_sem, recv_sem=recv_sem,
            device_id=device, device_id_type=MESH,
        )

    loads[0].wait()
    half = 2 * modes_y
    pair = 2
    for part in range(HALVES):

        def transform(step, carry, part=part):
            for offset in range(pair):
                local = step * pair + offset
                channel = part * group + local
                fetch(channel).wait()
                parts = []
                for plane in range(planes):
                    both = dot(y_table_ref[...], field[channel, plane])
                    y_values = both[:half] + both[half:]
                    parts += [y_values[:modes_y], y_values[modes_y:]]
                high, low = split(jnp.concatenate(parts, 1))
                rows = pl.ds(pl.multiple_of(local * modes_y, modes_y), modes_y)
                y_high[rows] = high
                y_low[rows] = low
            return carry

        lax.fori_loop(0, group // pair, transform, 0)
        if part == 0:
            loads[1].wait()
        both = dot(y_high[...], z_table_ref[...])
        value = both[:, :lanes] + both[:, lanes:] + dot(y_low[...], z_table_ref[:, :lanes])
        values_ref[part] = jnp.swapaxes(value.reshape(group, modes_y, lanes), 0, 1)

    spot = lax.broadcasted_iota(jnp.int32, (modes_y, group, lanes), 2)
    first, second = values_ref[0], values_ref[1]
    middle = lanes // HALVES
    spec[0] = jnp.where(spot < middle, first, pltpu.roll(second, middle, 2))
    spec[1] = jnp.where(spot < middle, pltpu.roll(first, middle, 2), second)

    for load in loads[2:10]:
        load.wait()
    rank_out = in_ref.shape[1]
    factor[...] = jnp.concatenate(
        [in_ref[...], out_ref[...], jnp.zeros((channels, lanes - 2 * rank_out), F32)], 1
    )
    y_wide = spread(y_ref[...], y_pick_ref[...], 0)
    row = lax.broadcasted_iota(jnp.int32, (same_ref.shape[0], y_wide.shape[0]), 0)
    spot = lax.broadcasted_iota(jnp.int32, row.shape, 1)
    rank_x = x_ref.shape[0]
    wanted = my_gx * width_col + lax.rem(lax.div(row, rank_x), width_col)
    y_high_rows, y_low_rows = split(
        spread(jnp.where(spot == wanted, 1.0, 0.0), y_wide, 1) * same_ref[...]
    )
    y_stack = jnp.concatenate([y_high_rows, y_low_rows], 0)
    core_rows = y_wide.shape[1]
    out_rows = same_ref.shape[0]
    rank_z = lanes // rank_out
    spot_rows = width_col * rank_x

    def contract(step, carry):
        rows = pl.ds(pl.multiple_of(step * core_rows, core_rows), core_rows)
        high, low = split(core_in[rows])
        both = dot(y_stack, high)
        value = both[:out_rows] + both[out_rows:] + dot(y_high_rows, low)
        wide = jnp.concatenate(
            [value[e * spot_rows : (e + 1) * spot_rows] for e in range(rank_z)], 1
        )
        place = pl.ds(pl.multiple_of(step * rank_x, rank_x), rank_x)
        for target in range(width_col):
            cores[target, place] = wide[target * rank_x : (target + 1) * rank_x]
        return carry

    lax.fori_loop(0, core_in.shape[0] // core_rows, contract, 0)

    pl.semaphore_wait(barrier, count - 1)

    def factor_copy(writer, device):
        return remote(
            factor, factors.at[writer], factor_sends.at[0], factor_recvs.at[writer], device
        )

    def core_copy(peer, writer, device):
        return remote(
            cores.at[peer], cores_in.at[writer], core_sends.at[0], core_recvs.at[writer], device
        )

    def send_half(part, source, target, send_sems, recv_sems):
        for gx_step in gx_steps:
            slab = slab_at(gx_step)
            for col_step in col_steps:
                if gx_step or col_step:
                    column = col_at(col_step)
                    remote(
                        source.at[part, slab * width_col + column], target.at[part, me],
                        send_sems.at[part], recv_sems.at[part, my_gx], (slab, column),
                    ).start()

    def receive(part, target, recv_sems, slab, messages):
        block = target.at[part, pl.ds(0, messages)]
        remote(block, block, recv_sems.at[part, slab], recv_sems.at[part, slab], (my_gx, my_col)
               ).wait_recv()

    for step in range(1, width_col):
        factor_copy(my_col, (my_gx, col_at(step))).start()
    send_half(0, spec, arrived, sends, recvs)
    for step in range(1, width_col):
        core_copy(col_at(step), my_col, (my_gx, col_at(step))).start()
    send_half(1, spec, arrived, sends, recvs)

    for part in range(HALVES):
        arrived[part, me] = spec[part, me]
    cores_in[my_col] = cores[my_col]
    factors[my_col] = factor[...]
    for load in loads[10:17]:
        load.wait()
    x_wide = spread(x_ref[...], x_pick_ref[...], 0)
    z_rows = spread(z_ref[...], z_pick_ref[...], 0)
    spot = lax.broadcasted_iota(jnp.int32, reach_ref.shape, 1)
    reach = jnp.where(spot == me, reach_ref[...].astype(F32), 0.0)
    reach = jnp.sum(reach, axis=1, keepdims=True)
    slot = lax.broadcasted_iota(jnp.int32, x_wide.shape, 0)
    slot = jnp.where(slot < modes_x // 2, slot, modes_x - slot).astype(F32)
    for l in range(modes_z):
        kept_ref[l] = jnp.where(slot < reach[l : l + 1], x_wide, 0.0)

    for step in range(1, width_col):
        factor_copy(col_at(step), (my_gx, my_col)).wait_recv()
    in_stack, out_parts = [], []
    for part in range(HALVES):
        rows = factors[:, part * group : (part + 1) * group].reshape(width_col * group, lanes)
        in_high, in_low = split(spread(rows[:, :rank_out], in_pick_ref[...], 1))
        in_stack += [in_high, in_low, in_high, in_low]
        out_parts.append(spread(rows[:, rank_out : 2 * rank_out], out_pick_ref[...], 1))
    in_stack = jnp.concatenate(in_stack, 0)
    out_high, out_low = split(jnp.concatenate(out_parts, 0))
    out_stack = jnp.concatenate([out_high, out_low], 0)
    rows_out = out_high.shape[0]

    lead = 2 * planes
    modes_half = modes_z // HALVES
    both_modes = 2 * modes_x
    ranks = x_wide.shape[1]
    last = (((1,), (1,)), ((), ()))

    def gather_ranks(part):
        for gx_step in gx_steps:
            slab = slab_at(gx_step)
            receive(part, arrived, recvs, slab, width_col if gx_step else width_col - 1)
            block = arrived[part, pl.ds(slab * width_col, width_col)]
            block = block.reshape(width_col * group, lanes)
            high = block.astype(BF16).astype(F32)
            low = block - high
            stacked = jnp.concatenate([high, high, low, low], 0).T.astype(BF16)
            wide = jnp.concatenate([stacked[:middle], stacked[middle:]], 1)
            value = dot(wide, in_stack).reshape(modes_half, lead, ranks)
            rank_ref[:, pl.ds(pl.multiple_of(slab * lead, lead), lead)] = value

    def mix(part, core_high, core_both):
        for l in range(modes_half):
            high, low = split(rank_ref[l])
            value = dot(fore_ref[...], jnp.concatenate([high, low, high], 0))
            kept = kept_ref[part * modes_half + l]
            value = value * jnp.concatenate([kept] * 4, 0)
            value = jnp.concatenate([value[:both_modes], value[both_modes:]], 1)
            rows = slice(l * both_modes, (l + 1) * both_modes)
            high_ref[rows], low_ref[rows] = split(value)
        both = dot(high_ref[...], core_both)
        mixed = both[:, :lanes] + both[:, lanes:] + dot(low_ref[...], core_high)
        for l in range(modes_half):
            at = part * modes_half + l
            value = mixed[l * both_modes : (l + 1) * both_modes] * z_rows[at : at + 1]
            high, low = split(value)
            value = dot(back_ref[...], jnp.concatenate([high, low, high], 0))
            plane_ref[:, l] = value.reshape(width_gx, lead, lanes)

    def expand(part):
        spot = lax.broadcasted_iota(jnp.int32, (rows_out // HALVES, lanes), 1)
        for slab in range(0, width_gx, HALVES):
            rows = plane_ref[slab : slab + HALVES].reshape(lanes, lanes)
            high, low = split(rows)
            both = lax.dot_general(out_stack, high, last, preferred_element_type=F32)
            value = both[:rows_out] + both[rows_out:]
            value = value + lax.dot_general(out_high, low, last, preferred_element_type=F32)
            first, second = value[: rows_out // HALVES], value[rows_out // HALVES :]
            pieces = (
                jnp.where(spot < middle, first, pltpu.roll(second, middle, 1)),
                jnp.where(spot < middle, pltpu.roll(first, middle, 1), second),
            )
            for offset, piece in enumerate(pieces):
                at = (slab + offset) * width_col
                result[part, at : at + width_col] = piece.reshape(width_col, group, lanes)

    for part in range(HALVES):
        gather_ranks(part)
        if part == 0:
            for step in range(1, width_col):
                core_copy(my_col, col_at(step), (my_gx, my_col)).wait_recv()
            half_rows = cores.shape[1] // 2
            core = [cores_in[:, first : first + half_rows] for first in (0, half_rows)]
            core = jnp.concatenate([rows.reshape(ranks, lanes) for rows in core], 0)
            core_high, core_low = split(core)
            core_both = jnp.concatenate([core_high, core_low], 1)
        mix(part, core_high, core_both)
        expand(part)
        send_half(part, result, returned, back_sends, back_recvs)
        returned[part, me] = result[part, me]

    loads[17].wait()
    ky_half = modes_y // 2
    gx_half = width_gx // 2
    my_half = lax.div(my_gx, gx_half)
    spot = lax.broadcasted_iota(jnp.int32, (group * ky_half, lanes), 1)
    wide = 2 * grid_z
    for part in range(HALVES):
        for turn in range(2):
            side = lax.rem(my_half + turn, 2)
            for step in range(gx_half):
                slab = side * gx_half + lax.rem(my_gx + step, gx_half)
                full = turn > 0 or step > 0
                receive(part, returned, back_recvs, slab, width_col if full else width_col - 1)
            block = returned[part, pl.ds(side * ky_half, ky_half)]
            block = jnp.swapaxes(block, 0, 1).reshape(group * ky_half, lanes)
            high = block.astype(BF16).astype(F32)
            low = block - high
            high_turned, low_turned = pltpu.roll(high, middle, 1), pltpu.roll(low, middle, 1)
            one = [jnp.where(spot < middle, high, low_turned), high[:, :middle]]
            two = [jnp.where(spot < middle, high_turned, low), high_turned[:, :middle]]
            stacked = jnp.concatenate(
                [jnp.concatenate(one, 1), jnp.concatenate(two, 1)], 0
            ).astype(BF16)
            rows = pl.ds(pl.multiple_of(side * ky_half, ky_half), ky_half)
            for plane in range(planes):
                at = slice(plane * wide, (plane + 1) * wide)
                value = dot(stacked, z_back_ref[part, :, at]).reshape(channels, ky_half, wide)
                if part + 1 < HALVES:
                    partial_ref[:, rows, at] = value
                else:
                    value = value + partial_ref[:, rows, at]
                    high_out[:, rows, at], low_out[:, rows, at] = split(value)

    loads[18].wait()
    for source, send_sem in ((factors, factor_sends.at[0]), (cores, core_sends.at[0])):
        block = source.at[pl.ds(0, width_col - 1)]
        remote(block, block, send_sem, send_sem, (my_gx, my_col)).wait_send()
    for part in range(HALVES):
        for target, send_sems in ((spec, sends), (result, back_sends)):
            block = target.at[part, pl.ds(0, count - 1)]
            remote(block, block, send_sems.at[part], send_sems.at[part], (my_gx, my_col)
                   ).wait_send()


def fused(
    grid_field, core, in_factor, out_factor, x_factor, y_factor, z_factor, kx_reach, width_gx,
    width_col,
):
    channels, planes, grid_y, grid_z = grid_field.shape
    modes_x, rank_x = x_factor.shape
    modes_y, rank_y = y_factor.shape
    modes_z, rank_z = z_factor.shape
    rank_in, rank_out = in_factor.shape[1], out_factor.shape[1]
    y_table, z_table = forward_tables(grid_y, grid_z, modes_y, modes_z, planes)
    y_back, z_back = inverse_tables(grid_y, grid_z, modes_y, modes_z, planes, HALVES)
    fore, back = x_tables(planes * width_gx, modes_x)
    picks = selectors(width_col, rank_in, rank_x, rank_y, rank_z, rank_out)
    count = width_gx * width_col
    lanes, wide = planes * 2 * modes_z, planes * 2 * grid_z
    ranks = rank_in * rank_x
    group = channels // HALVES
    dma = pltpu.SemaphoreType.DMA
    tables = [jnp.asarray(t) for t in picks + [y_table, z_table, fore, back, z_back, y_back]]
    small = [in_factor, out_factor, x_factor.T, y_factor.T, z_factor.T, kx_reach.T]
    operands = [grid_field, core] + small + tables
    core_rows = 2 * rank_in // width_col * rank_x
    exchange = (HALVES, count, group, lanes)
    return pl.pallas_call(
        functools.partial(fused_kernel, width_gx, width_col),
        out_shape=[
            pltpu.VMEM((channels, modes_y, wide), BF16),
            pltpu.VMEM((channels, modes_y, wide), BF16),
            pltpu.VMEM(y_back.shape, BF16),
        ],
        in_specs=[pl.BlockSpec(memory_space=pltpu.HBM)] * len(operands),
        out_specs=[VMEM] * 3,
        scratch_shapes=[pltpu.VMEM(a.shape, a.dtype) for a in operands[:-1]]
        + [
            pltpu.VMEM((group * modes_y, wide), BF16),
            pltpu.VMEM((group * modes_y, wide), BF16),
            pltpu.VMEM((HALVES, modes_y, group, lanes), F32),
            pltpu.VMEM(exchange, F32),
            pltpu.VMEM(exchange, F32),
            pltpu.VMEM((width_col, core_rows, lanes), F32),
            pltpu.VMEM((width_col, core_rows, lanes), F32),
            pltpu.VMEM((channels, lanes), F32),
            pltpu.VMEM((width_col, channels, lanes), F32),
            pltpu.VMEM((modes_z, modes_x, ranks), F32),
            pltpu.VMEM((modes_z // HALVES, 2 * planes * width_gx, ranks), F32),
            pltpu.VMEM((modes_z // HALVES * 2 * modes_x, 2 * ranks), BF16),
            pltpu.VMEM((modes_z // HALVES * 2 * modes_x, 2 * ranks), BF16),
            pltpu.VMEM((width_gx, modes_z // HALVES, 2 * planes, lanes), F32),
            pltpu.VMEM(exchange, F32),
            pltpu.VMEM(exchange, F32),
            pltpu.VMEM((channels, modes_y, wide), F32),
            dma((channels,)),
            dma((len(operands) - 1,)),
            dma((HALVES,)),
            dma((HALVES, width_gx)),
            dma((1,)),
            dma((width_col,)),
            dma((1,)),
            dma((width_col,)),
            dma((HALVES,)),
            dma((HALVES, width_gx)),
        ],
        compiler_params=pltpu.CompilerParams(
            collective_id=0, has_side_effects=True, vmem_limit_bytes=VMEM_BYTES
        ),
    )(*[pltpu.with_memory_space_constraint(a, pltpu.HBM) for a in operands])


VMEM_BYTES = 40 * 2**20
INVERSE_BYTES = 16 * 2**20


def inverse_kernel(high_ref, low_ref, y_ref, out_hbm, out, sems):
    channels, planes, _, grid_z = out.shape

    def tall(values, plane):
        at = 2 * plane * grid_z
        return [values[:, at : at + grid_z], values[:, at + grid_z : at + 2 * grid_z]]

    def leave(channel):
        return pltpu.make_async_copy(out.at[channel], out_hbm.at[channel], sems.at[channel])

    def transform(channel, carry):
        high, low = high_ref[channel], low_ref[channel]
        stacks = []
        for plane in range(planes):
            high_part = tall(high, plane)
            stacks.append(jnp.concatenate(high_part + tall(low, plane) + high_part, 0))
        for plane in range(0, planes, 2):
            value = dot(y_ref[...], jnp.concatenate(stacks[plane : plane + 2], 1)).astype(BF16)
            out[channel, plane] = value[:, :grid_z]
            out[channel, plane + 1] = value[:, grid_z:]
        leave(channel).start()
        return carry

    lax.fori_loop(0, channels, transform, 0)

    def finish(channel, carry):
        leave(channel).wait()
        return carry

    lax.fori_loop(0, channels, finish, 0)


def inverse(high, low, y_table, shape):
    return pl.pallas_call(
        inverse_kernel,
        in_specs=[VMEM] * 3,
        out_specs=pl.BlockSpec(memory_space=pltpu.HBM),
        out_shape=jax.ShapeDtypeStruct(shape, BF16),
        scratch_shapes=[pltpu.VMEM(shape, BF16), pltpu.SemaphoreType.DMA((shape[0],))],
        compiler_params=pltpu.CompilerParams(vmem_limit_bytes=INVERSE_BYTES),
    )(*[pltpu.with_memory_space_constraint(a, pltpu.VMEM) for a in (high, low, y_table)])


def row_device(
    grid_field, tucker_core, in_factor, out_factor, x_factor, y_factor, z_factor, kx_reach
):
    width_gx, width_col = lax.axis_size("gx"), lax.axis_size("col")
    rank_out = out_factor.shape[1]
    core = jnp.transpose(tucker_core, (0, 1, 3, 4, 5, 2)).reshape(-1, rank_out)
    high, low, y_table = fused(
        grid_field, core, in_factor, out_factor, x_factor, y_factor, z_factor, kx_reach, width_gx,
        width_col,
    )
    return inverse(high, low, y_table, grid_field.shape)


def per_device(
    grid_field, tucker_core, in_factor, out_factor, x_factor, y_factor, z_factor, kx_reach
):
    planes, grid_z = grid_field.shape[1], grid_field.shape[3]
    modes_y, modes_z = y_factor.shape[0], z_factor.shape[0]
    devices = lax.axis_size("gx") * lax.axis_size("col")
    ranks = in_factor.shape[1] * x_factor.shape[1]
    row_each = (
        devices == modes_y
        and planes == 4
        and grid_field.shape[0] == 16
        and grid_z == 128
        and planes * 2 * modes_z == 128
        and ranks == 256
        and x_factor.shape[1] == 8
        and in_factor.shape[1] == out_factor.shape[1]
        and y_factor.shape[1] * x_factor.shape[1] * z_factor.shape[1] == 256
        and out_factor.shape[1] * z_factor.shape[1] == 128
    )
    device = row_device if row_each else plain_device
    return device(
        grid_field, tucker_core, in_factor, out_factor, x_factor, y_factor, z_factor, kx_reach
    )


def solution(mesh):
    return jax.shard_map(
        per_device,
        mesh=mesh,
        in_specs=(
            P("col", "gx", None, None),
            P(None, "col", None, None, None, None),
            P("col", None),
            P("col", None),
            P(),
            P(),
            P(),
            P(),
        ),
        out_specs=P("col", "gx", None, None),
        check_vma=False,
    )
```

```python
import functools
import math

import jax
import jax.numpy as jnp
import numpy as np
from jax import lax
from jax.experimental import pallas as pl
from jax.experimental.pallas import tpu as pltpu
from jax.sharding import PartitionSpec as P

MESH = pl.DeviceIdType.MESH
VMEM = pl.BlockSpec(memory_space=pltpu.VMEM)
F32 = jnp.float32
BF16 = jnp.bfloat16


def slot_freq(slot_count):
    slot_index = jnp.arange(slot_count, dtype=jnp.int32)
    return jnp.where(slot_index < slot_count // 2, slot_index, slot_index - slot_count)


def phase_table(positions, extent, slot_count, direction):
    phase_steps = positions[:, None] * slot_freq(slot_count)[None, :] % extent
    radians = 2.0 * math.pi / extent * phase_steps.astype(jnp.float32)
    norm_scale = 1.0 / math.sqrt(extent)
    cosine = jnp.cos(radians) * norm_scale
    sine_part = direction * jnp.sin(radians) * norm_scale
    return jnp.stack([jnp.stack([cosine, -sine_part], 1), jnp.stack([sine_part, cosine], 1)], 1)


def z_tables(grid_z, modes_z):
    z_index = jnp.arange(grid_z, dtype=jnp.int32)
    kz_index = jnp.arange(modes_z, dtype=jnp.int32)
    phase_steps = z_index[:, None] * kz_index[None, :] % grid_z
    radians = 2.0 * math.pi / grid_z * phase_steps.astype(jnp.float32)
    norm_scale = 1.0 / math.sqrt(grid_z)
    cosine = jnp.cos(radians) * norm_scale
    sine_part = jnp.sin(radians) * norm_scale
    forward = jnp.stack([cosine, -sine_part], 1)
    weight = jnp.where(kz_index == 0, 1.0, 2.0).astype(jnp.float32)
    backward = jnp.stack([(cosine * weight[None, :]).T, -(sine_part * weight[None, :]).T], 0)
    return (forward, backward)


def plain_device(
    grid_field, tucker_core, in_factor, out_factor, x_factor, y_factor, z_factor, kx_reach
):
    highest = lax.Precision.HIGHEST
    channels, planes, grid_y, grid_z = grid_field.shape
    modes_x = x_factor.shape[0]
    modes_y = y_factor.shape[0]
    modes_z = z_factor.shape[0]
    width_gx = lax.axis_size("gx")
    grid_x = planes * width_gx
    columns = modes_y * modes_z
    col_dev = columns // width_gx
    slab_index = lax.axis_index("gx")
    z_forward, z_backward = z_tables(grid_z, modes_z)
    y_forward = phase_table(jnp.arange(grid_y, dtype=jnp.int32), grid_y, modes_y, 1.0)
    x_forward = phase_table(jnp.arange(grid_x, dtype=jnp.int32), grid_x, modes_x, 1.0)
    values = grid_field.astype(jnp.float32)
    z_spectrum = jnp.einsum("cxyz,zpl->cxply", values, z_forward, precision=highest)
    y_spectrum = jnp.einsum("cxply,ypqj->qcxjl", z_spectrum, y_forward, precision=highest)
    y_spectrum = y_spectrum.reshape(2, channels, planes, columns)
    first_col = slab_index * col_dev
    reach_dev = lax.dynamic_slice_in_dim(kx_reach.reshape(-1), first_col, col_dev)
    kept_mask = (jnp.abs(slot_freq(modes_x))[:, None] < reach_dev[None, :]).astype(jnp.float32)
    arrived = lax.all_to_all(y_spectrum, "gx", split_axis=3, concat_axis=2, tiled=True)
    spectrum = jnp.einsum("pcxm,xpqk->qckm", arrived, x_forward, precision=highest)
    partial_value = jnp.einsum("qckm,cr->qrkm", spectrum, in_factor, precision=highest)
    amplitude = lax.psum_scatter(partial_value, "col", scatter_dimension=1, tiled=True)
    amplitude = amplitude * kept_mask[None, None]
    column = first_col + jnp.arange(col_dev, dtype=jnp.int32)
    pick_y = (column[:, None] // modes_z == jnp.arange(modes_y, dtype=jnp.int32)[None, :]).astype(
        jnp.float32
    )
    pick_z = (column[:, None] % modes_z == jnp.arange(modes_z, dtype=jnp.int32)[None, :]).astype(
        jnp.float32
    )
    y_rows = jnp.dot(pick_y, y_factor, precision=highest)
    z_rows = jnp.dot(pick_z, z_factor, precision=highest)
    core_cols = jnp.einsum("prsabe,mb,me->prsam", tucker_core, y_rows, z_rows, precision=highest)
    kernel = jnp.einsum("prsam,ka->prskm", core_cols, x_factor, precision=highest)
    mixed_re = jnp.einsum("rskm,rkm->skm", kernel[0], amplitude[0], precision=highest) - jnp.einsum(
        "rskm,rkm->skm", kernel[1], amplitude[1], precision=highest
    )
    mixed_im = jnp.einsum("rskm,rkm->skm", kernel[0], amplitude[1], precision=highest) + jnp.einsum(
        "rskm,rkm->skm", kernel[1], amplitude[0], precision=highest
    )
    mixed_sum = lax.psum(jnp.stack([mixed_re, mixed_im]), "col")
    out_spec = jnp.einsum("os,qskm->qokm", out_factor, mixed_sum, precision=highest)
    x_backward = phase_table(jnp.arange(grid_x, dtype=jnp.int32), grid_x, modes_x, -1.0)
    x_values = jnp.einsum("pckm,xpqk->qcxm", out_spec, x_backward, precision=highest)
    returned = lax.all_to_all(x_values, "gx", split_axis=2, concat_axis=3, tiled=True)
    returned = returned.reshape(2, channels, planes, modes_y, modes_z)
    y_backward = phase_table(jnp.arange(grid_y, dtype=jnp.int32), grid_y, modes_y, -1.0)
    y_values = jnp.einsum("pcxjl,ypqj->cxqly", returned, y_backward, precision=highest)
    result = jnp.einsum("cxqly,qlz->cxyz", y_values, z_backward, precision=highest)
    return result.astype(jnp.bfloat16)


def split_np(table):
    high = table.astype(np.float32).astype(BF16)
    low = (table - high.astype(np.float64)).astype(np.float32).astype(BF16)
    return high, low


def split(values):
    high = values.astype(BF16)
    return high, (values - high.astype(F32)).astype(BF16)


def freqs(slots):
    index = np.arange(slots)
    return np.where(index < slots // 2, index, index - slots)


def waves(extent, frequencies):
    steps = np.arange(extent)[:, None] * frequencies[None, :] % extent
    angle = 2.0 * np.pi / extent * steps
    return np.cos(angle) / math.sqrt(extent), np.sin(angle) / math.sqrt(extent)


def dot(a, b):
    return jnp.dot(a, b, preferred_element_type=F32)


def forward_tables(grid_y, grid_z, modes_y, modes_z, planes):
    cos_y, sin_y = waves(grid_y, freqs(modes_y))
    high, low = split_np(np.concatenate([cos_y.T, -sin_y.T], 0))
    y_table = np.concatenate([high, low], 0)
    cos_z, sin_z = waves(grid_z, np.arange(modes_z))
    table = np.zeros((planes, 2, grid_z, modes_z, planes, 2))
    for plane in range(planes):
        table[plane, 0, :, :, plane, 0] = cos_z
        table[plane, 0, :, :, plane, 1] = -sin_z
        table[plane, 1, :, :, plane, 0] = sin_z
        table[plane, 1, :, :, plane, 1] = cos_z
    high, low = split_np(table.reshape(planes * 2 * grid_z, -1))
    return y_table, np.concatenate([high, low], 1)


def inverse_tables(grid_y, grid_z, modes_y, modes_z, planes):
    cos_y, sin_y = waves(grid_y, freqs(modes_y))
    high, low = split_np(np.concatenate([cos_y, -sin_y], 1))
    y_table = np.concatenate([high, high, low], 1)
    cos_z, sin_z = waves(grid_z, np.arange(modes_z))
    weight = np.where(np.arange(modes_z) == 0, 1.0, 2.0)
    cos_z, sin_z = (cos_z * weight).T, (sin_z * weight).T
    table = np.zeros((modes_z, planes, 2, planes, 2, grid_z))
    for plane in range(planes):
        table[:, plane, 0, plane, 0, :] = cos_z
        table[:, plane, 1, plane, 0, :] = -sin_z
        table[:, plane, 0, plane, 1, :] = sin_z
        table[:, plane, 1, plane, 1, :] = cos_z
    high, low = split_np(table.reshape(modes_z, planes * 2, -1))
    z_tables = []
    for first, modes in mode_chunks(modes_z):
        parts = [part[first : first + modes] for part in (high, high, low)]
        z_tables.append(np.concatenate(parts, 0).reshape(3 * modes * planes * 2, -1))
    return y_table, z_tables


def x_tables(grid_x, modes_x):
    cos_x, sin_x = waves(grid_x, freqs(modes_x))
    real = np.stack([cos_x.T, sin_x.T], 2).reshape(modes_x, -1)
    imag = np.stack([-sin_x.T, cos_x.T], 2).reshape(modes_x, -1)
    high, low = split_np(np.concatenate([real, imag], 0))
    forward = np.concatenate([high, high, low], 1)
    real = np.concatenate([cos_x, -sin_x], 1)
    imag = np.concatenate([sin_x, cos_x], 1)
    high, low = split_np(np.stack([real, imag], 1).reshape(grid_x * 2, -1))
    backward = np.concatenate([high, high, low], 1)
    return forward, backward


def selectors(width_col, rank_in, rank_x, rank_y, rank_z, rank_out):
    wide = np.arange(rank_in * rank_x)
    x_pick = wide % rank_x == np.arange(rank_x)[:, None]
    in_pick = wide // rank_x == np.arange(rank_in)[:, None]
    slim = np.arange(rank_z * rank_out)
    z_pick = slim // rank_out == np.arange(rank_z)[:, None]
    out_pick = slim % rank_out == np.arange(rank_out)[:, None]
    core_in = np.arange(rank_x * rank_y * rank_z)
    y_pick = core_in // rank_z % rank_y == np.arange(rank_y)[:, None]
    core_out = np.arange(rank_z * width_col * rank_x)
    same_x = core_in // (rank_y * rank_z) == core_out[:, None] % rank_x
    same_z = core_in % rank_z == core_out[:, None] // (width_col * rank_x)
    picks = (x_pick, in_pick, z_pick, out_pick, y_pick, same_x & same_z)
    return [pick.astype(np.float32) for pick in picks]


def spread(values, pick, dim):
    return lax.dot_general(
        values, pick, (((dim,), (0,)), ((), ())), precision=lax.Precision.HIGHEST,
        preferred_element_type=F32,
    )


SHARES = (1, 1)


def mode_chunks(modes_z):
    sizes = [share * modes_z // sum(SHARES) for share in SHARES]
    return [(sum(sizes[:chunk]), size) for chunk, size in enumerate(sizes)]


def blend(pieces, width):
    block = lax.broadcasted_iota(jnp.int32, pieces[0].shape, pieces[0].ndim - 1)
    value = pieces[0]
    for index, piece in enumerate(pieces[1:], 1):
        value = jnp.where(block >= index * width, piece, value)
    return value


def turn(values, shift):
    lanes = values.shape[-1]
    return pltpu.roll(values, shift % lanes, values.ndim - 1) if shift % lanes else values


def fused_kernel(
    width_gx, width_col, field_hbm, core_hbm, in_hbm, out_hbm, x_hbm, y_hbm, z_hbm, reach_hbm,
    x_pick_hbm, in_pick_hbm, z_pick_hbm, out_pick_hbm, y_pick_hbm, same_hbm, y_table_hbm,
    z_table_hbm, fore_hbm, back_hbm, y_back_hbm, *refs,
):
    chunks = len(SHARES)
    z_back_hbm, refs = refs[:chunks], refs[chunks:]
    high_out, low_out, y_back_ref, *refs = refs
    field, core_in, in_ref, out_ref, x_ref, y_ref, z_ref, reach_ref, *refs = refs
    x_pick_ref, in_pick_ref, z_pick_ref, out_pick_ref, y_pick_ref, same_ref, *refs = refs
    y_table_ref, z_table_ref, fore_ref, back_ref, *refs = refs
    z_back_ref, refs = refs[:chunks], refs[chunks:]
    spec, refs = refs[:chunks], refs[chunks:]
    arrived, refs = refs[:chunks], refs[chunks:]
    result, refs = refs[:chunks], refs[chunks:]
    returned, refs = refs[:chunks], refs[chunks:]
    y_high, y_low, values_ref, cores, cores_in, factor, factors, kept_ref, rank_ref, *refs = refs
    plane_ref, partial_ref, field_sems, load_sems, sends, recvs, *refs = refs
    core_sends, core_recvs, factor_sends, factor_recvs, back_sends, back_recvs = refs
    count = width_gx * width_col
    my_gx, my_col = lax.axis_index("gx"), lax.axis_index("col")
    me = my_gx * width_col + my_col
    channels, planes, _, grid_z = field.shape
    _, modes_y, lanes = values_ref.shape
    modes_x, modes_z = x_ref.shape[1], z_ref.shape[1]
    lead = 2 * planes
    barrier = pltpu.get_barrier_semaphore()
    gx_steps = sorted(range(width_gx), key=lambda step: min(step, width_gx - step))
    near = gx_steps[: width_gx // 2]
    col_steps = range(width_col)

    def slab_at(step):
        return lax.rem(my_gx + step, width_gx)

    def col_at(step):
        return lax.rem(my_col + step, width_col)

    for gx_step in gx_steps:
        for col_step in col_steps:
            if gx_step or col_step:
                pl.semaphore_signal(
                    barrier, inc=1, device_id=(slab_at(gx_step), col_at(col_step)),
                    device_id_type=MESH,
                )

    burst = channels // field_sems.shape[0]

    def fetch(channel):
        return pltpu.make_async_copy(
            field_hbm.at[channel], field.at[channel], field_sems.at[lax.div(channel, burst)]
        )

    stages = [
        [(y_table_hbm, y_table_ref)],
        [(z_table_hbm, z_table_ref)],
        [(in_hbm, in_ref), (out_hbm, out_ref), (y_hbm, y_ref), (y_pick_hbm, y_pick_ref),
         (same_hbm, same_ref)],
        [(core_hbm, core_in)],
        [(in_pick_hbm, in_pick_ref), (out_pick_hbm, out_pick_ref), (x_hbm, x_ref), (z_hbm, z_ref),
         (reach_hbm, reach_ref), (x_pick_hbm, x_pick_ref), (z_pick_hbm, z_pick_ref),
         (fore_hbm, fore_ref), (back_hbm, back_ref)],
        [(y_back_hbm, y_back_ref), *zip(z_back_hbm, z_back_ref)],
    ]
    loads = [
        [pltpu.make_async_copy(source, target, load_sems.at[stage]) for source, target in copies]
        for stage, copies in enumerate(stages)
    ]

    def await_loads(stage):
        for load in loads[stage]:
            load.wait()

    loads[0][0].start()

    def begin(channel, carry):
        fetch(channel).start()
        return carry

    lax.fori_loop(0, channels, begin, 0)
    for stage in loads[1:]:
        for load in stage:
            load.start()

    def remote(source, target, send_sem, recv_sem, device):
        return pltpu.make_async_remote_copy(
            src_ref=source, dst_ref=target, send_sem=send_sem, recv_sem=recv_sem,
            device_id=device, device_id_type=MESH,
        )

    await_loads(0)
    half = 2 * modes_y
    batch = channels // 2
    for part in range(2):

        def transform(step, carry, part=part):
            first = part * batch + step * burst
            pltpu.make_async_copy(
                field_hbm.at[pl.ds(first, burst)], field.at[pl.ds(first, burst)],
                field_sems.at[lax.div(first, burst)],
            ).wait()
            for offset in range(burst):
                local = step * burst + offset
                channel = first + offset
                parts = []
                for plane in range(0, planes, 2):
                    two = jnp.concatenate([field[channel, plane], field[channel, plane + 1]], 1)
                    both = dot(y_table_ref[...], two)
                    y_values = both[:half] + both[half:]
                    for at in (0, grid_z):
                        parts += [
                            y_values[:modes_y, at : at + grid_z],
                            y_values[modes_y:, at : at + grid_z],
                        ]
                high, low = split(jnp.concatenate(parts, 1))
                rows = pl.ds(pl.multiple_of(local * modes_y, modes_y), modes_y)
                y_high[rows] = high
                y_low[rows] = low
            return carry

        lax.fori_loop(0, batch // burst, transform, 0)
        if part == 0:
            await_loads(1)
        both = dot(y_high[...], z_table_ref[...])
        value = both[:, :lanes] + both[:, lanes:] + dot(y_low[...], z_table_ref[:, :lanes])
        values_ref[part * batch : (part + 1) * batch] = value.reshape(batch, modes_y, lanes)

    sizes = []
    for first, modes in mode_chunks(modes_z):
        width = modes * lead
        groups = lanes // width
        sizes.append((first, modes, width, groups, channels // groups))

    def pack(chunk):
        first, _, width, groups, rows = sizes[chunk]
        pieces = [
            turn(values_ref[g * rows : (g + 1) * rows], g * width - first * lead)
            for g in range(groups)
        ]
        spec[chunk][...] = jnp.swapaxes(blend(pieces, width), 0, 1)

    pack(0)
    await_loads(2)
    rank_out = in_ref.shape[1]
    factor[...] = jnp.concatenate(
        [in_ref[...], out_ref[...], jnp.zeros((channels, lanes - 2 * rank_out), F32)], 1
    )
    y_wide = spread(y_ref[...], y_pick_ref[...], 0)
    row = lax.broadcasted_iota(jnp.int32, (same_ref.shape[0], y_wide.shape[0]), 0)
    spot = lax.broadcasted_iota(jnp.int32, row.shape, 1)
    rank_x = x_ref.shape[0]
    wanted = my_gx * width_col + lax.rem(lax.div(row, rank_x), width_col)
    y_rows = spread(jnp.where(spot == wanted, 1.0, 0.0), y_wide, 1) * same_ref[...]
    y_stack = jnp.concatenate(split(y_rows), 0)
    out_rows, core_rows = y_rows.shape
    rank_z = lanes // rank_out
    spot_rows = width_col * rank_x

    pl.semaphore_wait(barrier, count - 1)

    def factor_copy(writer, device):
        return remote(
            factor, factors.at[writer], factor_sends.at[0], factor_recvs.at[0], device
        )

    def core_copy(peer, writer, device):
        return remote(
            cores.at[peer], cores_in.at[writer], core_sends.at[0], core_recvs.at[0], device
        )

    def near_side(gx_step):
        return 0 if (width_gx - gx_step) % width_gx in near else 1

    def own_side(gx_step):
        return lax.div(my_gx, width_gx // 2)

    def send_chunk(chunk, source, target, send_sems, recv_sems, side_of):
        for gx_step in gx_steps:
            slab = slab_at(gx_step)
            for col_step in col_steps:
                if gx_step or col_step:
                    column = col_at(col_step)
                    remote(
                        source[chunk].at[slab * width_col + column], target[chunk].at[me],
                        send_sems.at[chunk], recv_sems.at[chunk, side_of(gx_step)], (slab, column),
                    ).start()

    def receive(chunk, target, recv_sem, messages):
        block = target[chunk].at[pl.ds(0, messages)]
        remote(block, block, recv_sem, recv_sem, (my_gx, my_col)).wait_recv()

    send_chunk(0, spec, arrived, sends, recvs, near_side)
    for step in range(1, width_col):
        factor_copy(my_col, (my_gx, col_at(step))).start()
    await_loads(3)
    for step in range(0, core_in.shape[0] // core_rows, rank_z):
        tall = [core_in[(step + e) * core_rows : (step + e + 1) * core_rows] for e in range(rank_z)]
        high, low = split(jnp.concatenate(tall, 1))
        value = dot(y_stack, jnp.concatenate([high, low], 1))
        value = value[:out_rows] + value[out_rows:]
        value = value[:, :lanes] + value[:, lanes:]
        for offset in range(rank_z):
            pieces = [
                turn(value[e * spot_rows : (e + 1) * spot_rows], (e - offset) * rank_out)
                for e in range(rank_z)
            ]
            wide = blend(pieces, rank_out)
            first = (step + offset) * rank_x
            for target in range(width_col):
                rows = wide[target * rank_x : (target + 1) * rank_x]
                cores[target, first : first + rank_x] = rows

    for step in range(1, width_col):
        core_copy(col_at(step), my_col, (my_gx, col_at(step))).start()
    pack(1)
    send_chunk(1, spec, arrived, sends, recvs, near_side)

    await_loads(4)
    x_wide = spread(x_ref[...], x_pick_ref[...], 0)
    z_rows = spread(z_ref[...], z_pick_ref[...], 0)
    spot = lax.broadcasted_iota(jnp.int32, reach_ref.shape, 1)
    reach = jnp.where(spot == me, reach_ref[...].astype(F32), 0.0)
    reach = jnp.sum(reach, axis=1, keepdims=True)
    slot = lax.broadcasted_iota(jnp.int32, x_wide.shape, 0)
    slot = jnp.where(slot < modes_x // 2, slot, modes_x - slot).astype(F32)
    for l in range(modes_z):
        kept_ref[l] = jnp.where(slot < reach[l : l + 1], x_wide, 0.0)
    for chunk in range(2, chunks):
        pack(chunk)
        send_chunk(chunk, spec, arrived, sends, recvs, near_side)
    for chunk in range(chunks):
        arrived[chunk][me] = spec[chunk][me]
    cores_in[my_col] = cores[my_col]
    factors[my_col] = factor[...]

    others = factors.at[pl.ds(0, width_col - 1)]
    remote(others, others, factor_recvs.at[0], factor_recvs.at[0], (my_gx, my_col)).wait_recv()
    rows = factors[...].reshape(width_col * channels, lanes)
    in_rows = spread(rows[:, :rank_out], in_pick_ref[...], 1)
    out_all = spread(rows[:, rank_out : 2 * rank_out], out_pick_ref[...], 1)

    def regroup(values, groups):
        values = values.reshape(width_col, groups, channels // groups, -1)
        return [values[:, g].reshape(width_col * channels // groups, -1) for g in range(groups)]

    in_stacks, out_stacks = {}, {}
    for groups in sorted({size[3] for size in sizes}):
        stack = []
        for in_group in regroup(in_rows, groups):
            in_high, in_low = split(in_group)
            stack += [in_high, in_low, in_high, in_low]
        in_stacks[groups] = jnp.concatenate(stack, 0)
        out_stacks[groups] = split(jnp.concatenate(regroup(out_all, groups), 0))
    rows_out = out_all.shape[0]

    both_modes = 2 * modes_x
    ranks = x_wide.shape[1]
    last = (((1,), (1,)), ((), ()))

    def gather_ranks(chunk):
        _, modes, width, groups, rows = sizes[chunk]
        copies = lanes // (4 * width_col * rows)
        if chunk:
            receive(chunk, arrived, recvs.at[chunk, 0], count // 2 - 1)
            receive(chunk, arrived, recvs.at[chunk, 1], count // 2)
            turns = [gx_steps]
        else:
            turns = [near, gx_steps[width_gx // 2 :]]
        for side, steps in enumerate(turns):
            if not chunk:
                receive(chunk, arrived, recvs.at[chunk, side], count // 2 - 1 + side)
            for gx_step in steps:
                slab = slab_at(gx_step)
                block = arrived[chunk][pl.ds(slab * width_col, width_col)]
                block = block.reshape(width_col * rows, lanes)
                stacked = []
                for copy in range(copies):
                    high, low = split(turn(block, -copy * width))
                    stacked += [high, high, low, low]
                stacked = jnp.concatenate(stacked, 0).T
                wide = [
                    stacked[g * width : (g + 1) * width] for g in range(0, groups, copies)
                ]
                value = dot(jnp.concatenate(wide, 1), in_stacks[groups])
                value = value.reshape(modes, lead, ranks)
                rank_ref[:modes, pl.ds(pl.multiple_of(slab * lead, lead), lead)] = value

    def mix(chunk, core_high, core_low):
        first, modes = sizes[chunk][:2]
        parts = []
        for l in range(modes):
            high, low = split(rank_ref[l])
            value = dot(fore_ref[...], jnp.concatenate([high, low, high], 0))
            parts.append(split(value * jnp.concatenate([kept_ref[first + l]] * 2, 0)))
        mixed = []
        for start in (0, modes // 2):
            high, low = (
                jnp.concatenate(rows, 0) for rows in zip(*parts[start : start + modes // 2])
            )
            mixed.append(dot(high, core_high) + dot(low, core_high) + dot(high, core_low))
        for l in range(modes):
            both = mixed[l // (modes // 2)]
            at = l % (modes // 2) * both_modes
            real, imag = both[at : at + modes_x], both[at + modes_x : at + both_modes]
            value = jnp.concatenate(
                [real[:, :lanes] - imag[:, lanes:], real[:, lanes:] + imag[:, :lanes]], 0
            )
            high, low = split(value * z_rows[first + l : first + l + 1])
            value = dot(back_ref[...], jnp.concatenate([high, low, high], 0))
            plane_ref[:, l] = value.reshape(width_gx, lead, lanes)

    def expand(chunk):
        _, modes, width, groups, rows = sizes[chunk]
        out_high, out_low = out_stacks[groups]
        out_stack = jnp.concatenate([out_high, out_low], 0)
        group_rows = width_col * rows
        for slab in range(0, width_gx, groups):
            high, low = split(plane_ref[slab : slab + groups, :modes].reshape(lanes, lanes))
            both = lax.dot_general(out_stack, high, last, preferred_element_type=F32)
            value = both[:rows_out] + both[rows_out:]
            value = value + lax.dot_general(out_high, low, last, preferred_element_type=F32)
            for offset in range(groups):
                pieces = [
                    turn(value[g * group_rows : (g + 1) * group_rows], (g - offset) * width)
                    for g in range(groups)
                ]
                at = (slab + offset) * width_col
                piece = blend(pieces, width).reshape(width_col, rows, lanes)
                result[chunk][at : at + width_col] = piece

    for chunk in range(chunks):
        gather_ranks(chunk)
        if chunk == 0:
            others = cores_in.at[pl.ds(0, width_col - 1)]
            remote(others, others, core_recvs.at[0], core_recvs.at[0], (my_gx, my_col)).wait_recv()
            half_rows = cores.shape[1] // 2
            core = [cores_in[:, first : first + half_rows] for first in (0, half_rows)]
            core = jnp.concatenate([rows.reshape(ranks, lanes) for rows in core], 1)
            core_high, core_low = split(core)
        mix(chunk, core_high, core_low)
        expand(chunk)
        send_chunk(chunk, result, returned, back_sends, back_recvs, own_side)
        returned[chunk][me] = result[chunk][me]

    await_loads(5)
    ky_half = modes_y // 2
    gx_half = width_gx // 2
    my_half = lax.div(my_gx, gx_half)
    wide = 2 * grid_z
    for chunk in range(chunks):
        _, _, width, groups, rows = sizes[chunk]
        for side_step in range(2):
            side = lax.rem(my_half + side_step, 2)
            receive(chunk, returned, back_recvs.at[chunk, side], count // 2 - 1 + side_step)
            block = returned[chunk][pl.ds(side * ky_half, ky_half)]
            block = jnp.swapaxes(block, 0, 1).reshape(rows * ky_half, lanes)
            high = block.astype(BF16).astype(F32)
            low = block - high
            stacked = []
            for g in range(groups):
                pieces = [
                    turn(value, (spot - g) * width) for spot, value in enumerate((high, low, high))
                ]
                tiles = [
                    blend(pieces[tile : tile + groups], width) for tile in range(0, 3, groups)
                ]
                stacked.append(jnp.concatenate(tiles, 1)[:, : 3 * width])
            stacked = jnp.concatenate(stacked, 0).astype(BF16)
            spots = pl.ds(pl.multiple_of(side * ky_half, ky_half), ky_half)
            for plane in range(planes):
                at = slice(plane * wide, (plane + 1) * wide)
                value = dot(stacked, z_back_ref[chunk][:, at]).reshape(channels, ky_half, wide)
                if chunk > 0:
                    value = value + partial_ref[:, spots, at]
                if chunk + 1 < chunks:
                    partial_ref[:, spots, at] = value
                else:
                    high_out[:, spots, at], low_out[:, spots, at] = split(value)

    for source, send_sem in ((factors, factor_sends.at[0]), (cores, core_sends.at[0])):
        block = source.at[pl.ds(0, width_col - 1)]
        remote(block, block, send_sem, send_sem, (my_gx, my_col)).wait_send()
    for chunk in range(chunks):
        for target, send_sems in ((spec, sends), (result, back_sends)):
            block = target[chunk].at[pl.ds(0, count - 1)]
            sem = send_sems.at[chunk]
            remote(block, block, sem, sem, (my_gx, my_col)).wait_send()


def fused(
    grid_field, core, in_factor, out_factor, x_factor, y_factor, z_factor, kx_reach, width_gx,
    width_col,
):
    channels, planes, grid_y, grid_z = grid_field.shape
    modes_x, rank_x = x_factor.shape
    modes_y, rank_y = y_factor.shape
    modes_z, rank_z = z_factor.shape
    rank_in, rank_out = in_factor.shape[1], out_factor.shape[1]
    y_table, z_table = forward_tables(grid_y, grid_z, modes_y, modes_z, planes)
    y_back, z_back = inverse_tables(grid_y, grid_z, modes_y, modes_z, planes)
    fore, back = x_tables(planes * width_gx, modes_x)
    picks = selectors(width_col, rank_in, rank_x, rank_y, rank_z, rank_out)
    count = width_gx * width_col
    lanes, wide = planes * 2 * modes_z, planes * 2 * grid_z
    ranks = rank_in * rank_x
    dma = pltpu.SemaphoreType.DMA
    chunks = mode_chunks(modes_z)
    most = max(modes for _, modes in chunks)
    exchange = [
        pltpu.VMEM((count, channels * modes // modes_z, lanes), F32) for _, modes in chunks
    ]
    tables = [jnp.asarray(t) for t in picks + [y_table, z_table, fore, back, y_back] + z_back]
    small = [in_factor, out_factor, x_factor.T, y_factor.T, z_factor.T, kx_reach.T]
    operands = [grid_field, core] + small + tables
    keep = len(operands) - len(chunks) - 1
    loaded = operands[:keep] + operands[keep + 1 :]
    core_rows = 2 * rank_in // width_col * rank_x
    return pl.pallas_call(
        functools.partial(fused_kernel, width_gx, width_col),
        out_shape=[
            pltpu.VMEM((channels, modes_y, wide), BF16),
            pltpu.VMEM((channels, modes_y, wide), BF16),
            pltpu.VMEM(y_back.shape, BF16),
        ],
        in_specs=[pl.BlockSpec(memory_space=pltpu.HBM)] * len(operands),
        out_specs=[VMEM] * 3,
        scratch_shapes=[pltpu.VMEM(a.shape, a.dtype) for a in loaded]
        + exchange * 4
        + [
            pltpu.VMEM((channels // 2 * modes_y, wide), BF16),
            pltpu.VMEM((channels // 2 * modes_y, wide), BF16),
            pltpu.VMEM((channels, modes_y, lanes), F32),
            pltpu.VMEM((width_col, core_rows, lanes), F32),
            pltpu.VMEM((width_col, core_rows, lanes), F32),
            pltpu.VMEM((channels, lanes), F32),
            pltpu.VMEM((width_col, channels, lanes), F32),
            pltpu.VMEM((modes_z, modes_x, ranks), F32),
            pltpu.VMEM((most, 2 * planes * width_gx, ranks), F32),
            pltpu.VMEM((width_gx, most, 2 * planes, lanes), F32),
            pltpu.VMEM((channels, modes_y, wide), F32),
            dma((4,)),
            dma((6,)),
            dma((len(chunks),)),
            dma((len(chunks), 2)),
            dma((1,)),
            dma((1,)),
            dma((1,)),
            dma((1,)),
            dma((len(chunks),)),
            dma((len(chunks), 2)),
        ],
        compiler_params=pltpu.CompilerParams(
            collective_id=0, has_side_effects=True, vmem_limit_bytes=VMEM_BYTES
        ),
    )(*[pltpu.with_memory_space_constraint(a, pltpu.HBM) for a in operands])


VMEM_BYTES = 40 * 2**20
INVERSE_BYTES = 16 * 2**20
INVERSE_UNROLL = 8


def inverse_kernel(high_ref, low_ref, y_ref, out_hbm, out, sems):
    channels, planes, _, grid_z = out.shape

    def tall(values, plane):
        at = 2 * plane * grid_z
        return [values[:, at : at + grid_z], values[:, at + grid_z : at + 2 * grid_z]]

    def leave(channel):
        return pltpu.make_async_copy(out.at[channel], out_hbm.at[channel], sems.at[channel])

    def transform(channel, carry):
        high, low = high_ref[channel], low_ref[channel]
        stacks = []
        for plane in range(planes):
            high_part = tall(high, plane)
            stacks.append(jnp.concatenate(high_part + tall(low, plane) + high_part, 0))
        for plane in range(0, planes, 2):
            value = dot(y_ref[...], jnp.concatenate(stacks[plane : plane + 2], 1)).astype(BF16)
            out[channel, plane] = value[:, :grid_z]
            out[channel, plane + 1] = value[:, grid_z:]
        leave(channel).start()
        return carry

    lax.fori_loop(0, channels, transform, 0, unroll=INVERSE_UNROLL)

    def finish(channel, carry):
        leave(channel).wait()
        return carry

    lax.fori_loop(0, channels, finish, 0)


def inverse(high, low, y_table, shape):
    return pl.pallas_call(
        inverse_kernel,
        in_specs=[VMEM] * 3,
        out_specs=pl.BlockSpec(memory_space=pltpu.HBM),
        out_shape=jax.ShapeDtypeStruct(shape, BF16),
        scratch_shapes=[pltpu.VMEM(shape, BF16), pltpu.SemaphoreType.DMA((shape[0],))],
        compiler_params=pltpu.CompilerParams(vmem_limit_bytes=INVERSE_BYTES),
    )(*[pltpu.with_memory_space_constraint(a, pltpu.VMEM) for a in (high, low, y_table)])


def row_device(
    grid_field, tucker_core, in_factor, out_factor, x_factor, y_factor, z_factor, kx_reach
):
    width_gx, width_col = lax.axis_size("gx"), lax.axis_size("col")
    rank_out = out_factor.shape[1]
    core = jnp.transpose(tucker_core, (0, 1, 3, 4, 5, 2)).reshape(-1, rank_out)
    high, low, y_table = fused(
        grid_field, core, in_factor, out_factor, x_factor, y_factor, z_factor, kx_reach, width_gx,
        width_col,
    )
    return inverse(high, low, y_table, grid_field.shape)


def per_device(
    grid_field, tucker_core, in_factor, out_factor, x_factor, y_factor, z_factor, kx_reach
):
    planes, grid_z = grid_field.shape[1], grid_field.shape[3]
    modes_y, modes_z = y_factor.shape[0], z_factor.shape[0]
    devices = lax.axis_size("gx") * lax.axis_size("col")
    ranks = in_factor.shape[1] * x_factor.shape[1]
    row_each = (
        devices == modes_y
        and planes == 4
        and grid_field.shape[0] == 16
        and grid_z == 128
        and planes * 2 * modes_z == 128
        and ranks == 256
        and x_factor.shape[1] == 8
        and in_factor.shape[1] == out_factor.shape[1]
        and y_factor.shape[1] * x_factor.shape[1] * z_factor.shape[1] == 256
        and out_factor.shape[1] * z_factor.shape[1] == 128
    )
    device = row_device if row_each else plain_device
    return device(
        grid_field, tucker_core, in_factor, out_factor, x_factor, y_factor, z_factor, kx_reach
    )


def solution(mesh):
    return jax.shard_map(
        per_device,
        mesh=mesh,
        in_specs=(
            P("col", "gx", None, None),
            P(None, "col", None, None, None, None),
            P("col", None),
            P("col", None),
            P(),
            P(),
            P(),
            P(),
        ),
        out_specs=P("col", "gx", None, None),
        check_vma=False,
    )
```

```python
import functools
import math

import jax
import jax.numpy as jnp
import numpy as np
from jax import lax
from jax.experimental import pallas as pl
from jax.experimental.pallas import tpu as pltpu
from jax.sharding import PartitionSpec as P

MESH = pl.DeviceIdType.MESH
VMEM = pl.BlockSpec(memory_space=pltpu.VMEM)
F32 = jnp.float32
BF16 = jnp.bfloat16


def slot_freq(slot_count):
    slot_index = jnp.arange(slot_count, dtype=jnp.int32)
    return jnp.where(slot_index < slot_count // 2, slot_index, slot_index - slot_count)


def phase_table(positions, extent, slot_count, direction):
    phase_steps = positions[:, None] * slot_freq(slot_count)[None, :] % extent
    radians = 2.0 * math.pi / extent * phase_steps.astype(jnp.float32)
    norm_scale = 1.0 / math.sqrt(extent)
    cosine = jnp.cos(radians) * norm_scale
    sine_part = direction * jnp.sin(radians) * norm_scale
    return jnp.stack([jnp.stack([cosine, -sine_part], 1), jnp.stack([sine_part, cosine], 1)], 1)


def z_tables(grid_z, modes_z):
    z_index = jnp.arange(grid_z, dtype=jnp.int32)
    kz_index = jnp.arange(modes_z, dtype=jnp.int32)
    phase_steps = z_index[:, None] * kz_index[None, :] % grid_z
    radians = 2.0 * math.pi / grid_z * phase_steps.astype(jnp.float32)
    norm_scale = 1.0 / math.sqrt(grid_z)
    cosine = jnp.cos(radians) * norm_scale
    sine_part = jnp.sin(radians) * norm_scale
    forward = jnp.stack([cosine, -sine_part], 1)
    weight = jnp.where(kz_index == 0, 1.0, 2.0).astype(jnp.float32)
    backward = jnp.stack([(cosine * weight[None, :]).T, -(sine_part * weight[None, :]).T], 0)
    return (forward, backward)


def plain_device(
    grid_field, tucker_core, in_factor, out_factor, x_factor, y_factor, z_factor, kx_reach
):
    highest = lax.Precision.HIGHEST
    channels, planes, grid_y, grid_z = grid_field.shape
    modes_x = x_factor.shape[0]
    modes_y = y_factor.shape[0]
    modes_z = z_factor.shape[0]
    width_gx = lax.axis_size("gx")
    grid_x = planes * width_gx
    columns = modes_y * modes_z
    col_dev = columns // width_gx
    slab_index = lax.axis_index("gx")
    z_forward, z_backward = z_tables(grid_z, modes_z)
    y_forward = phase_table(jnp.arange(grid_y, dtype=jnp.int32), grid_y, modes_y, 1.0)
    x_forward = phase_table(jnp.arange(grid_x, dtype=jnp.int32), grid_x, modes_x, 1.0)
    values = grid_field.astype(jnp.float32)
    z_spectrum = jnp.einsum("cxyz,zpl->cxply", values, z_forward, precision=highest)
    y_spectrum = jnp.einsum("cxply,ypqj->qcxjl", z_spectrum, y_forward, precision=highest)
    y_spectrum = y_spectrum.reshape(2, channels, planes, columns)
    first_col = slab_index * col_dev
    reach_dev = lax.dynamic_slice_in_dim(kx_reach.reshape(-1), first_col, col_dev)
    kept_mask = (jnp.abs(slot_freq(modes_x))[:, None] < reach_dev[None, :]).astype(jnp.float32)
    arrived = lax.all_to_all(y_spectrum, "gx", split_axis=3, concat_axis=2, tiled=True)
    spectrum = jnp.einsum("pcxm,xpqk->qckm", arrived, x_forward, precision=highest)
    partial_value = jnp.einsum("qckm,cr->qrkm", spectrum, in_factor, precision=highest)
    amplitude = lax.psum_scatter(partial_value, "col", scatter_dimension=1, tiled=True)
    amplitude = amplitude * kept_mask[None, None]
    column = first_col + jnp.arange(col_dev, dtype=jnp.int32)
    pick_y = (column[:, None] // modes_z == jnp.arange(modes_y, dtype=jnp.int32)[None, :]).astype(
        jnp.float32
    )
    pick_z = (column[:, None] % modes_z == jnp.arange(modes_z, dtype=jnp.int32)[None, :]).astype(
        jnp.float32
    )
    y_rows = jnp.dot(pick_y, y_factor, precision=highest)
    z_rows = jnp.dot(pick_z, z_factor, precision=highest)
    core_cols = jnp.einsum("prsabe,mb,me->prsam", tucker_core, y_rows, z_rows, precision=highest)
    kernel = jnp.einsum("prsam,ka->prskm", core_cols, x_factor, precision=highest)
    mixed_re = jnp.einsum("rskm,rkm->skm", kernel[0], amplitude[0], precision=highest) - jnp.einsum(
        "rskm,rkm->skm", kernel[1], amplitude[1], precision=highest
    )
    mixed_im = jnp.einsum("rskm,rkm->skm", kernel[0], amplitude[1], precision=highest) + jnp.einsum(
        "rskm,rkm->skm", kernel[1], amplitude[0], precision=highest
    )
    mixed_sum = lax.psum(jnp.stack([mixed_re, mixed_im]), "col")
    out_spec = jnp.einsum("os,qskm->qokm", out_factor, mixed_sum, precision=highest)
    x_backward = phase_table(jnp.arange(grid_x, dtype=jnp.int32), grid_x, modes_x, -1.0)
    x_values = jnp.einsum("pckm,xpqk->qcxm", out_spec, x_backward, precision=highest)
    returned = lax.all_to_all(x_values, "gx", split_axis=2, concat_axis=3, tiled=True)
    returned = returned.reshape(2, channels, planes, modes_y, modes_z)
    y_backward = phase_table(jnp.arange(grid_y, dtype=jnp.int32), grid_y, modes_y, -1.0)
    y_values = jnp.einsum("pcxjl,ypqj->cxqly", returned, y_backward, precision=highest)
    result = jnp.einsum("cxqly,qlz->cxyz", y_values, z_backward, precision=highest)
    return result.astype(jnp.bfloat16)


def split_np(table):
    high = table.astype(np.float32).astype(BF16)
    low = (table - high.astype(np.float64)).astype(np.float32).astype(BF16)
    return high, low


def split(values):
    high = values.astype(BF16)
    return high, (values - high.astype(F32)).astype(BF16)


def freqs(slots):
    index = np.arange(slots)
    return np.where(index < slots // 2, index, index - slots)


def waves(extent, frequencies):
    steps = np.arange(extent)[:, None] * frequencies[None, :] % extent
    angle = 2.0 * np.pi / extent * steps
    return np.cos(angle) / math.sqrt(extent), np.sin(angle) / math.sqrt(extent)


def dot(a, b):
    return jnp.dot(a, b, preferred_element_type=F32)


def forward_tables(grid_y, grid_z, modes_y, modes_z, planes):
    cos_y, sin_y = waves(grid_y, freqs(modes_y))
    high, low = split_np(np.concatenate([cos_y.T, -sin_y.T], 0))
    y_table = np.concatenate([high, low], 0)
    cos_z, sin_z = waves(grid_z, np.arange(modes_z))
    table = np.zeros((planes, 2, grid_z, modes_z, planes, 2))
    for plane in range(planes):
        table[plane, 0, :, :, plane, 0] = cos_z
        table[plane, 0, :, :, plane, 1] = -sin_z
        table[plane, 1, :, :, plane, 0] = sin_z
        table[plane, 1, :, :, plane, 1] = cos_z
    high, low = split_np(table.reshape(planes * 2 * grid_z, -1))
    return y_table, np.concatenate([high, low], 1)


def inverse_tables(grid_y, grid_z, modes_y, modes_z, planes):
    cos_y, sin_y = waves(grid_y, freqs(modes_y))
    high, low = split_np(np.concatenate([cos_y, -sin_y], 1))
    y_table = np.concatenate([high, high, low], 1)
    cos_z, sin_z = waves(grid_z, np.arange(modes_z))
    weight = np.where(np.arange(modes_z) == 0, 1.0, 2.0)
    cos_z, sin_z = (cos_z * weight).T, (sin_z * weight).T
    table = np.zeros((modes_z, planes, 2, planes, 2, grid_z))
    for plane in range(planes):
        table[:, plane, 0, plane, 0, :] = cos_z
        table[:, plane, 1, plane, 0, :] = -sin_z
        table[:, plane, 0, plane, 1, :] = sin_z
        table[:, plane, 1, plane, 1, :] = cos_z
    high, low = split_np(table.reshape(modes_z, planes * 2, -1))
    chunks = mode_chunks(modes_z)
    z_tables = []
    for family in families(modes_z):
        parts = []
        for first, modes in [chunks[chunk] for chunk in family]:
            parts += [part[first : first + modes] for part in (high, high, low)]
        z_tables.append(np.concatenate(parts, 0).reshape(-1, high.shape[-1]))
    return y_table, z_tables


def x_tables(grid_x, modes_x):
    cos_x, sin_x = waves(grid_x, freqs(modes_x))
    real = np.stack([cos_x.T, sin_x.T], 2).reshape(modes_x, -1)
    imag = np.stack([-sin_x.T, cos_x.T], 2).reshape(modes_x, -1)
    high, low = split_np(np.concatenate([real, imag], 0))
    forward = np.concatenate([high, high, low], 1)
    real = np.concatenate([cos_x, -sin_x], 1)
    imag = np.concatenate([sin_x, cos_x], 1)
    high, low = split_np(np.stack([real, imag], 1).reshape(grid_x * 2, -1))
    backward = np.concatenate([high, high, low], 1)
    return forward, backward


def selectors(width_col, rank_in, rank_x, rank_y, rank_z, rank_out):
    wide = np.arange(rank_in * rank_x)
    x_pick = wide % rank_x == np.arange(rank_x)[:, None]
    in_pick = wide // rank_x == np.arange(rank_in)[:, None]
    slim = np.arange(rank_z * rank_out)
    z_pick = slim // rank_out == np.arange(rank_z)[:, None]
    out_pick = slim % rank_out == np.arange(rank_out)[:, None]
    core_in = np.arange(rank_x * rank_y * rank_z)
    y_pick = core_in // rank_z % rank_y == np.arange(rank_y)[:, None]
    core_out = np.arange(rank_z * width_col * rank_x)
    same_x = core_in // (rank_y * rank_z) == core_out[:, None] % rank_x
    same_z = core_in % rank_z == core_out[:, None] // (width_col * rank_x)
    picks = (x_pick, in_pick, z_pick, out_pick, y_pick, same_x & same_z)
    return [pick.astype(np.float32) for pick in picks]


def spread(values, pick, dim):
    return lax.dot_general(
        values, pick, (((dim,), (0,)), ((), ())), precision=lax.Precision.HIGHEST,
        preferred_element_type=F32,
    )


SHARES = (1, 1)


def mode_chunks(modes_z):
    sizes = [share * modes_z // sum(SHARES) for share in SHARES]
    return [(sum(sizes[:chunk]), size) for chunk, size in enumerate(sizes)]


def families(modes_z):
    groups = []
    for chunk, (first, _) in enumerate(mode_chunks(modes_z)):
        if 2 * first % modes_z == 0:
            groups.append([])
        groups[-1].append(chunk)
    return groups


def blend(pieces, width):
    block = lax.broadcasted_iota(jnp.int32, pieces[0].shape, pieces[0].ndim - 1)
    value = pieces[0]
    for index, piece in enumerate(pieces[1:], 1):
        value = jnp.where(block >= index * width, piece, value)
    return value


def turn(values, shift):
    lanes = values.shape[-1]
    return pltpu.roll(values, shift % lanes, values.ndim - 1) if shift % lanes else values


def fused_kernel(
    width_gx, width_col, field_hbm, core_hbm, in_hbm, out_hbm, x_hbm, y_hbm, z_hbm, reach_hbm,
    x_pick_hbm, in_pick_hbm, z_pick_hbm, out_pick_hbm, y_pick_hbm, same_hbm, y_table_hbm,
    z_table_hbm, fore_hbm, back_hbm, y_back_hbm, *refs,
):
    chunks = len(SHARES)
    parts = len(families(sum(SHARES)))
    z_back_hbm, refs = refs[:parts], refs[parts:]
    high_out, low_out, y_back_ref, *refs = refs
    field, core_in, in_ref, out_ref, x_ref, y_ref, z_ref, reach_ref, *refs = refs
    x_pick_ref, in_pick_ref, z_pick_ref, out_pick_ref, y_pick_ref, same_ref, *refs = refs
    y_table_ref, z_table_ref, fore_ref, back_ref, *refs = refs
    z_back_ref, refs = refs[: len(z_back_hbm)], refs[len(z_back_hbm) :]
    spec, refs = refs[:chunks], refs[chunks:]
    arrived, refs = refs[:chunks], refs[chunks:]
    result, refs = refs[:chunks], refs[chunks:]
    returned, refs = refs[:chunks], refs[chunks:]
    y_high, y_low, values_ref, cores, cores_in, factor, factors, kept_ref, rank_ref, *refs = refs
    plane_ref, partial_ref, field_sems, load_sems, sends, recvs, *refs = refs
    core_sends, core_recvs, factor_sends, factor_recvs, back_sends, back_recvs = refs
    count = width_gx * width_col
    my_gx, my_col = lax.axis_index("gx"), lax.axis_index("col")
    me = my_gx * width_col + my_col
    channels, planes, _, grid_z = field.shape
    _, modes_y, lanes = values_ref.shape
    modes_x, modes_z = x_ref.shape[1], z_ref.shape[1]
    lead = 2 * planes
    barrier = pltpu.get_barrier_semaphore()
    gx_steps = sorted(range(width_gx), key=lambda step: min(step, width_gx - step))
    near = gx_steps[: width_gx // 2]
    col_steps = range(width_col)

    def slab_at(step):
        return lax.rem(my_gx + step, width_gx)

    def col_at(step):
        return lax.rem(my_col + step, width_col)

    burst = channels // field_sems.shape[0]

    def fetch(channel):
        return pltpu.make_async_copy(
            field_hbm.at[channel], field.at[channel], field_sems.at[lax.div(channel, burst)]
        )

    stages = [
        [(y_hbm, y_ref), (y_pick_hbm, y_pick_ref), (same_hbm, same_ref)],
        [(y_table_hbm, y_table_ref)],
        [(z_table_hbm, z_table_ref), (in_hbm, in_ref), (out_hbm, out_ref)],
        [(core_hbm, core_in)],
        [(in_pick_hbm, in_pick_ref), (out_pick_hbm, out_pick_ref), (x_hbm, x_ref), (z_hbm, z_ref),
         (reach_hbm, reach_ref), (x_pick_hbm, x_pick_ref), (z_pick_hbm, z_pick_ref),
         (fore_hbm, fore_ref), (back_hbm, back_ref)],
        [(y_back_hbm, y_back_ref), *zip(z_back_hbm, z_back_ref)],
    ]
    loads = [
        [pltpu.make_async_copy(source, target, load_sems.at[stage]) for source, target in copies]
        for stage, copies in enumerate(stages)
    ]

    def await_loads(stage):
        for load in loads[stage]:
            load.wait()

    def begin(first, after):
        for channel in range(first, min(first + channels // 2, channels)):
            fetch(channel).start()
        for stage in after:
            for load in loads[stage]:
                load.start()

    for load in loads[0] + loads[1]:
        load.start()
    begin(0, [])
    for gx_step in gx_steps:
        for col_step in col_steps:
            if gx_step or col_step:
                pl.semaphore_signal(
                    barrier, inc=1, device_id=(slab_at(gx_step), col_at(col_step)),
                    device_id_type=MESH,
                )

    def remote(source, target, send_sem, recv_sem, device):
        return pltpu.make_async_remote_copy(
            src_ref=source, dst_ref=target, send_sem=send_sem, recv_sem=recv_sem,
            device_id=device, device_id_type=MESH,
        )

    begin(channels // 2, [2])
    rank_out = in_ref.shape[1]
    await_loads(1)
    half = 2 * modes_y
    batch = channels // 2
    for part in range(2):

        def transform(step, carry, part=part):
            first = part * batch + step * burst
            pltpu.make_async_copy(
                field_hbm.at[pl.ds(first, burst)], field.at[pl.ds(first, burst)],
                field_sems.at[lax.div(first, burst)],
            ).wait()
            for offset in range(burst):
                local = step * burst + offset
                channel = first + offset
                parts = []
                for plane in range(0, planes, 2):
                    two = jnp.concatenate([field[channel, plane], field[channel, plane + 1]], 1)
                    both = dot(y_table_ref[...], two)
                    y_values = both[:half] + both[half:]
                    for at in (0, grid_z):
                        parts += [
                            y_values[:modes_y, at : at + grid_z],
                            y_values[modes_y:, at : at + grid_z],
                        ]
                high, low = split(jnp.concatenate(parts, 1))
                rows = pl.ds(pl.multiple_of(local * modes_y, modes_y), modes_y)
                y_high[rows] = high
                y_low[rows] = low
            return carry

        lax.fori_loop(0, batch // burst, transform, 0)
        if part == 0:
            begin(channels, [3, 4, 5])
            await_loads(2)
        both = dot(y_high[...], z_table_ref[...])
        value = both[:, :lanes] + both[:, lanes:] + dot(y_low[...], z_table_ref[:, :lanes])
        values_ref[part * batch : (part + 1) * batch] = value.reshape(batch, modes_y, lanes)

    sizes = []
    for first, modes in mode_chunks(modes_z):
        width = modes * lead
        groups = lanes // width
        sizes.append((first, modes, width, groups, channels // groups))

    def pack(chunk):
        first, _, width, groups, rows = sizes[chunk]
        pieces = [
            turn(values_ref[g * rows : (g + 1) * rows], g * width - first * lead)
            for g in range(groups)
        ]
        spec[chunk][...] = jnp.swapaxes(blend(pieces, width), 0, 1)

    pack(0)
    factor[...] = jnp.concatenate(
        [in_ref[...], out_ref[...], jnp.zeros((channels, lanes - 2 * rank_out), F32)], 1
    )
    pl.semaphore_wait(barrier, count - 1)

    def factor_copy(writer, device):
        return remote(
            factor, factors.at[writer], factor_sends.at[0], factor_recvs.at[0], device
        )

    def core_copy(peer, writer, device):
        return remote(
            cores.at[peer], cores_in.at[writer], core_sends.at[0], core_recvs.at[0], device
        )

    def near_side(gx_step):
        return 0 if (width_gx - gx_step) % width_gx in near else 1

    def own_side(gx_step):
        return lax.div(my_gx, width_gx // 2)

    def send_chunk(chunk, source, target, send_sems, recv_sems, side_of):
        for gx_step in gx_steps:
            slab = slab_at(gx_step)
            for col_step in col_steps:
                if gx_step or col_step:
                    column = col_at(col_step)
                    remote(
                        source[chunk].at[slab * width_col + column], target[chunk].at[me],
                        send_sems.at[chunk], recv_sems.at[chunk, side_of(gx_step)], (slab, column),
                    ).start()

    def receive(chunk, target, recv_sem, messages):
        block = target[chunk].at[pl.ds(0, messages)]
        remote(block, block, recv_sem, recv_sem, (my_gx, my_col)).wait_recv()

    send_chunk(0, spec, arrived, sends, recvs, near_side)
    for step in range(1, width_col):
        factor_copy(my_col, (my_gx, col_at(step))).start()
    await_loads(0)
    y_wide = spread(y_ref[...], y_pick_ref[...], 0)
    row = lax.broadcasted_iota(jnp.int32, (same_ref.shape[0], y_wide.shape[0]), 0)
    spot = lax.broadcasted_iota(jnp.int32, row.shape, 1)
    rank_x = x_ref.shape[0]
    wanted = my_gx * width_col + lax.rem(lax.div(row, rank_x), width_col)
    y_rows = spread(jnp.where(spot == wanted, 1.0, 0.0), y_wide, 1) * same_ref[...]
    y_stack = jnp.concatenate(split(y_rows), 0)
    out_rows, core_rows = y_rows.shape
    rank_z = lanes // rank_out
    spot_rows = width_col * rank_x

    await_loads(3)
    for step in range(0, core_in.shape[0] // core_rows, rank_z):
        tall = [core_in[(step + e) * core_rows : (step + e + 1) * core_rows] for e in range(rank_z)]
        high, low = split(jnp.concatenate(tall, 1))
        value = dot(y_stack, jnp.concatenate([high, low], 1))
        value = value[:out_rows] + value[out_rows:]
        value = value[:, :lanes] + value[:, lanes:]
        for offset in range(rank_z):
            pieces = [
                turn(value[e * spot_rows : (e + 1) * spot_rows], (e - offset) * rank_out)
                for e in range(rank_z)
            ]
            wide = blend(pieces, rank_out)
            first = (step + offset) * rank_x
            for target in range(width_col):
                rows = wide[target * rank_x : (target + 1) * rank_x]
                cores[target, first : first + rank_x] = rows

    for step in range(1, width_col):
        core_copy(col_at(step), my_col, (my_gx, col_at(step))).start()

    pack(1)
    send_chunk(1, spec, arrived, sends, recvs, near_side)
    await_loads(4)
    x_wide = spread(x_ref[...], x_pick_ref[...], 0)
    z_rows = spread(z_ref[...], z_pick_ref[...], 0)
    spot = lax.broadcasted_iota(jnp.int32, reach_ref.shape, 1)
    reach = jnp.where(spot == me, reach_ref[...].astype(F32), 0.0)
    reach = jnp.sum(reach, axis=1, keepdims=True)
    slot = lax.broadcasted_iota(jnp.int32, x_wide.shape, 0)
    slot = jnp.where(slot < modes_x // 2, slot, modes_x - slot).astype(F32)
    for l in range(modes_z):
        kept_ref[l] = jnp.where(slot < reach[l : l + 1], x_wide, 0.0)
    for chunk in range(2, chunks):
        pack(chunk)
        send_chunk(chunk, spec, arrived, sends, recvs, near_side)
    for chunk in range(chunks):
        arrived[chunk][me] = spec[chunk][me]
    cores_in[my_col] = cores[my_col]
    factors[my_col] = factor[...]

    others = factors.at[pl.ds(0, width_col - 1)]
    remote(others, others, factor_recvs.at[0], factor_recvs.at[0], (my_gx, my_col)).wait_recv()
    rows = factors[...].reshape(width_col * channels, lanes)
    in_rows = spread(rows[:, :rank_out], in_pick_ref[...], 1)
    out_all = spread(rows[:, rank_out : 2 * rank_out], out_pick_ref[...], 1)

    def regroup(values, groups):
        values = values.reshape(width_col, groups, channels // groups, -1)
        return [values[:, g].reshape(width_col * channels // groups, -1) for g in range(groups)]

    in_stacks, out_stacks = {}, {}
    for groups in sorted({size[3] for size in sizes}):
        stack = []
        for in_group in regroup(in_rows, groups):
            in_high, in_low = split(in_group)
            stack += [in_high, in_low, in_high, in_low]
        in_stacks[groups] = jnp.concatenate(stack, 0)
        out_stacks[groups] = split(jnp.concatenate(regroup(out_all, groups), 0))
    rows_out = out_all.shape[0]

    both_modes = 2 * modes_x
    ranks = x_wide.shape[1]
    last = (((1,), (1,)), ((), ()))

    def gather_ranks(chunk):
        _, modes, width, groups, rows = sizes[chunk]
        copies = lanes // (4 * width_col * rows)
        if chunk:
            receive(chunk, arrived, recvs.at[chunk, 0], count // 2 - 1)
            receive(chunk, arrived, recvs.at[chunk, 1], count // 2)
            turns = [gx_steps]
        else:
            turns = [near, gx_steps[width_gx // 2 :]]
        for side, steps in enumerate(turns):
            if not chunk:
                receive(chunk, arrived, recvs.at[chunk, side], count // 2 - 1 + side)
            for gx_step in steps:
                slab = slab_at(gx_step)
                block = arrived[chunk][pl.ds(slab * width_col, width_col)]
                block = block.reshape(width_col * rows, lanes)
                stacked = []
                for copy in range(copies):
                    high, low = split(turn(block, -copy * width))
                    stacked += [high, high, low, low]
                stacked = jnp.concatenate(stacked, 0).T
                wide = [
                    stacked[g * width : (g + 1) * width] for g in range(0, groups, copies)
                ]
                value = dot(jnp.concatenate(wide, 1), in_stacks[groups])
                value = value.reshape(modes, lead, ranks)
                rank_ref[:modes, pl.ds(pl.multiple_of(slab * lead, lead), lead)] = value

    def mix(chunk, core_high, core_low):
        first, modes = sizes[chunk][:2]
        parts = []
        for l in range(modes):
            high, low = split(rank_ref[l])
            value = dot(fore_ref[...], jnp.concatenate([high, low, high], 0))
            parts.append(split(value * jnp.concatenate([kept_ref[first + l]] * 2, 0)))
        mixed = []
        for start in (0, modes // 2):
            high, low = (
                jnp.concatenate(rows, 0) for rows in zip(*parts[start : start + modes // 2])
            )
            mixed.append(dot(high, core_high) + dot(low, core_high) + dot(high, core_low))
        for l in range(modes):
            both = mixed[l // (modes // 2)]
            at = l % (modes // 2) * both_modes
            real, imag = both[at : at + modes_x], both[at + modes_x : at + both_modes]
            value = jnp.concatenate(
                [real[:, :lanes] - imag[:, lanes:], real[:, lanes:] + imag[:, :lanes]], 0
            )
            high, low = split(value * z_rows[first + l : first + l + 1])
            value = dot(back_ref[...], jnp.concatenate([high, low, high], 0))
            plane_ref[:, l] = value.reshape(width_gx, lead, lanes)

    def expand(chunk):
        _, modes, width, groups, rows = sizes[chunk]
        out_high, out_low = out_stacks[groups]
        out_stack = jnp.concatenate([out_high, out_low], 0)
        group_rows = width_col * rows
        for slab in range(0, width_gx, groups):
            high, low = split(plane_ref[slab : slab + groups, :modes].reshape(lanes, lanes))
            both = lax.dot_general(out_stack, high, last, preferred_element_type=F32)
            value = both[:rows_out] + both[rows_out:]
            value = value + lax.dot_general(out_high, low, last, preferred_element_type=F32)
            for offset in range(groups):
                pieces = [
                    turn(value[g * group_rows : (g + 1) * group_rows], (g - offset) * width)
                    for g in range(groups)
                ]
                at = (slab + offset) * width_col
                piece = blend(pieces, width).reshape(width_col, rows, lanes)
                result[chunk][at : at + width_col] = piece

    for chunk in range(chunks):
        gather_ranks(chunk)
        if chunk == 0:
            others = cores_in.at[pl.ds(0, width_col - 1)]
            remote(others, others, core_recvs.at[0], core_recvs.at[0], (my_gx, my_col)).wait_recv()
            half_rows = cores.shape[1] // 2
            core = [cores_in[:, first : first + half_rows] for first in (0, half_rows)]
            core = jnp.concatenate([rows.reshape(ranks, lanes) for rows in core], 1)
            core_high, core_low = split(core)
        mix(chunk, core_high, core_low)
        expand(chunk)
        send_chunk(chunk, result, returned, back_sends, back_recvs, own_side)
        returned[chunk][me] = result[chunk][me]

    await_loads(5)
    ky_half = modes_y // 2
    gx_half = width_gx // 2
    my_half = lax.div(my_gx, gx_half)
    wide = 2 * grid_z
    for turn_at, family in enumerate(families(modes_z)):
        _, _, width, groups, rows = sizes[family[0]]
        for side_step in range(2):
            side = lax.rem(my_half + side_step, 2)
            sources = []
            for chunk in family:
                receive(chunk, returned, back_recvs.at[chunk, side], count // 2 - 1 + side_step)
                block = returned[chunk][pl.ds(side * ky_half, ky_half)]
                block = jnp.swapaxes(block, 0, 1).reshape(rows * ky_half, lanes)
                high = block.astype(BF16).astype(F32)
                sources += [high, block - high, high]
            stacked = []
            for g in range(groups):
                pieces = [
                    turn(value, (spot - g) * width) for spot, value in enumerate(sources)
                ]
                tiles = [
                    blend(pieces[tile : tile + groups], width)
                    for tile in range(0, len(pieces), groups)
                ]
                stacked.append(jnp.concatenate(tiles, 1)[:, : len(pieces) * width])
            stacked = jnp.concatenate(stacked, 0).astype(BF16)
            spots = pl.ds(pl.multiple_of(side * ky_half, ky_half), ky_half)
            for plane in range(planes):
                at = slice(plane * wide, (plane + 1) * wide)
                value = dot(stacked, z_back_ref[turn_at][:, at])
                value = value.reshape(channels, ky_half, wide)
                if turn_at > 0:
                    value = value + partial_ref[:, spots, at]
                if turn_at + 1 < len(z_back_ref):
                    partial_ref[:, spots, at] = value
                else:
                    high_out[:, spots, at], low_out[:, spots, at] = split(value)

    for source, send_sem in ((factors, factor_sends.at[0]), (cores, core_sends.at[0])):
        block = source.at[pl.ds(0, width_col - 1)]
        remote(block, block, send_sem, send_sem, (my_gx, my_col)).wait_send()
    for chunk in range(chunks):
        for target, send_sems in ((spec, sends), (result, back_sends)):
            block = target[chunk].at[pl.ds(0, count - 1)]
            sem = send_sems.at[chunk]
            remote(block, block, sem, sem, (my_gx, my_col)).wait_send()


def fused(
    grid_field, core, in_factor, out_factor, x_factor, y_factor, z_factor, kx_reach, width_gx,
    width_col,
):
    channels, planes, grid_y, grid_z = grid_field.shape
    modes_x, rank_x = x_factor.shape
    modes_y, rank_y = y_factor.shape
    modes_z, rank_z = z_factor.shape
    rank_in, rank_out = in_factor.shape[1], out_factor.shape[1]
    y_table, z_table = forward_tables(grid_y, grid_z, modes_y, modes_z, planes)
    y_back, z_back = inverse_tables(grid_y, grid_z, modes_y, modes_z, planes)
    fore, back = x_tables(planes * width_gx, modes_x)
    picks = selectors(width_col, rank_in, rank_x, rank_y, rank_z, rank_out)
    count = width_gx * width_col
    lanes, wide = planes * 2 * modes_z, planes * 2 * grid_z
    ranks = rank_in * rank_x
    dma = pltpu.SemaphoreType.DMA
    chunks = mode_chunks(modes_z)
    most = max(modes for _, modes in chunks)
    exchange = [
        pltpu.VMEM((count, channels * modes // modes_z, lanes), F32) for _, modes in chunks
    ]
    tables = [jnp.asarray(t) for t in picks + [y_table, z_table, fore, back, y_back] + z_back]
    small = [in_factor, out_factor, x_factor.T, y_factor.T, z_factor.T, kx_reach.T]
    operands = [grid_field, core] + small + tables
    keep = len(operands) - len(z_back) - 1
    loaded = operands[:keep] + operands[keep + 1 :]
    core_rows = 2 * rank_in // width_col * rank_x
    return pl.pallas_call(
        functools.partial(fused_kernel, width_gx, width_col),
        out_shape=[
            pltpu.VMEM((channels, modes_y, wide), BF16),
            pltpu.VMEM((channels, modes_y, wide), BF16),
            pltpu.VMEM(y_back.shape, BF16),
        ],
        in_specs=[pl.BlockSpec(memory_space=pltpu.HBM)] * len(operands),
        out_specs=[VMEM] * 3,
        scratch_shapes=[pltpu.VMEM(a.shape, a.dtype) for a in loaded]
        + exchange * 4
        + [
            pltpu.VMEM((channels // 2 * modes_y, wide), BF16),
            pltpu.VMEM((channels // 2 * modes_y, wide), BF16),
            pltpu.VMEM((channels, modes_y, lanes), F32),
            pltpu.VMEM((width_col, core_rows, lanes), F32),
            pltpu.VMEM((width_col, core_rows, lanes), F32),
            pltpu.VMEM((channels, lanes), F32),
            pltpu.VMEM((width_col, channels, lanes), F32),
            pltpu.VMEM((modes_z, modes_x, ranks), F32),
            pltpu.VMEM((most, 2 * planes * width_gx, ranks), F32),
            pltpu.VMEM((width_gx, most, 2 * planes, lanes), F32),
            pltpu.VMEM((channels, modes_y, wide), F32),
            dma((4,)),
            dma((6,)),
            dma((len(chunks),)),
            dma((len(chunks), 2)),
            dma((1,)),
            dma((1,)),
            dma((1,)),
            dma((1,)),
            dma((len(chunks),)),
            dma((len(chunks), 2)),
        ],
        compiler_params=pltpu.CompilerParams(
            collective_id=0, has_side_effects=True, vmem_limit_bytes=VMEM_BYTES
        ),
    )(*[pltpu.with_memory_space_constraint(a, pltpu.HBM) for a in operands])


VMEM_BYTES = 40 * 2**20
INVERSE_BYTES = 16 * 2**20
INVERSE_UNROLL = 8


def inverse_kernel(high_ref, low_ref, y_ref, out_hbm, out, sems):
    channels, planes, _, grid_z = out.shape

    def tall(values, plane):
        at = 2 * plane * grid_z
        return [values[:, at : at + grid_z], values[:, at + grid_z : at + 2 * grid_z]]

    def leave(channel):
        return pltpu.make_async_copy(out.at[channel], out_hbm.at[channel], sems.at[channel])

    def transform(channel, carry):
        high, low = high_ref[channel], low_ref[channel]
        stacks = []
        for plane in range(planes):
            high_part = tall(high, plane)
            stacks.append(jnp.concatenate(high_part + tall(low, plane) + high_part, 0))
        for plane in range(0, planes, 2):
            value = dot(y_ref[...], jnp.concatenate(stacks[plane : plane + 2], 1)).astype(BF16)
            out[channel, plane] = value[:, :grid_z]
            out[channel, plane + 1] = value[:, grid_z:]
        leave(channel).start()
        return carry

    lax.fori_loop(0, channels, transform, 0, unroll=INVERSE_UNROLL)

    def finish(channel, carry):
        leave(channel).wait()
        return carry

    lax.fori_loop(0, channels, finish, 0)


def inverse(high, low, y_table, shape):
    return pl.pallas_call(
        inverse_kernel,
        in_specs=[VMEM] * 3,
        out_specs=pl.BlockSpec(memory_space=pltpu.HBM),
        out_shape=jax.ShapeDtypeStruct(shape, BF16),
        scratch_shapes=[pltpu.VMEM(shape, BF16), pltpu.SemaphoreType.DMA((shape[0],))],
        compiler_params=pltpu.CompilerParams(vmem_limit_bytes=INVERSE_BYTES),
    )(*[pltpu.with_memory_space_constraint(a, pltpu.VMEM) for a in (high, low, y_table)])


def row_device(
    grid_field, tucker_core, in_factor, out_factor, x_factor, y_factor, z_factor, kx_reach
):
    width_gx, width_col = lax.axis_size("gx"), lax.axis_size("col")
    rank_out = out_factor.shape[1]
    core = jnp.transpose(tucker_core, (0, 1, 3, 4, 5, 2)).reshape(-1, rank_out)
    high, low, y_table = fused(
        grid_field, core, in_factor, out_factor, x_factor, y_factor, z_factor, kx_reach, width_gx,
        width_col,
    )
    return inverse(high, low, y_table, grid_field.shape)


def per_device(
    grid_field, tucker_core, in_factor, out_factor, x_factor, y_factor, z_factor, kx_reach
):
    planes, grid_z = grid_field.shape[1], grid_field.shape[3]
    modes_y, modes_z = y_factor.shape[0], z_factor.shape[0]
    devices = lax.axis_size("gx") * lax.axis_size("col")
    ranks = in_factor.shape[1] * x_factor.shape[1]
    row_each = (
        devices == modes_y
        and planes == 4
        and grid_field.shape[0] == 16
        and grid_z == 128
        and planes * 2 * modes_z == 128
        and ranks == 256
        and x_factor.shape[1] == 8
        and in_factor.shape[1] == out_factor.shape[1]
        and y_factor.shape[1] * x_factor.shape[1] * z_factor.shape[1] == 256
        and out_factor.shape[1] * z_factor.shape[1] == 128
    )
    device = row_device if row_each else plain_device
    return device(
        grid_field, tucker_core, in_factor, out_factor, x_factor, y_factor, z_factor, kx_reach
    )


def solution(mesh):
    return jax.shard_map(
        per_device,
        mesh=mesh,
        in_specs=(
            P("col", "gx", None, None),
            P(None, "col", None, None, None, None),
            P("col", None),
            P("col", None),
            P(),
            P(),
            P(),
            P(),
        ),
        out_specs=P("col", "gx", None, None),
        check_vma=False,
    )
```
